128 devices in a mesh: row: 8 (over z, x_lo), col: 16 (over x_hi, y, core).
Axes of the slice: x: 4 (x_hi: 2, x_lo: 2; x = x_hi * 2 + x_lo), y: 4, z: 4, core: 2. Of those that a mesh axis runs over, the one named last changes fastest.
Arguments:
- scene_tokens: bfloat16 [128, 1024, 180], P('row', 'col'), may hold values from -8 to 8
- block_qkv: bfloat16 [3, 180, 540], replicated, may hold values from -1.8 to 1.8
- block_proj: bfloat16 [3, 180, 180], replicated, may hold values from -0.4375 to 0.4375
- conv_squeeze: bfloat16 [3, 9, 180, 60], replicated, may hold values from -0.15625 to 0.15625
- conv_expand: bfloat16 [3, 9, 60, 180], replicated, may hold values from -0.25 to 0.25
- gate_down: bfloat16 [3, 180, 6], replicated, may hold values from -4 to 4
- gate_up: bfloat16 [3, 6, 180], replicated, may hold values from -6 to 6
- mlp_in: bfloat16 [4, 180, 360], replicated, may hold values from -0.4375 to 0.4375
- mlp_out: bfloat16 [4, 360, 180], replicated, may hold values from -0.3125 to 0.3125
- ocab_qkv: bfloat16 [180, 540], replicated, may hold values from -1.8 to 1.8
- ocab_proj: bfloat16 [180, 180], replicated, may hold values from -0.4375 to 0.4375
Outputs:
- refined: bfloat16 [128, 1024, 180], P('row', 'col')
The draws below stay inside these ranges and needn't reach their ends.
All inputs are finite; a program needn't handle non-finite values.
Results may differ from the reference program's by a relative error of at most 0.034.
Values may be sent and summed in bfloat16 or wider, within the bound.
A program may use at most 128 MiB of HBM per device.

```python
import math
import jax
import jax.numpy as jnp
from jax import lax

C = 180
HEADS = 6
WIN = 16
HID = 360
CC = 60
CS = 6
SHIFT = 8
OVL = 4
NH = 128
NW = 1024


def draw_attention(key, layers_count):
    drawn = jax.random.normal(jax.random.fold_in(key, 11), (layers_count, C, 3 * C), jnp.float32) * C ** (-0.5)
    drawn = jnp.clip(drawn, -6.0 * C ** (-0.5), 6.0 * C ** (-0.5))
    return drawn


def draw_block_qkv(key, part):
    return draw_attention(key, 3).astype(jnp.bfloat16)


def draw_ocab_qkv(key, part):
    return draw_attention(key, 1)[0].astype(jnp.bfloat16)


def draw_scene_tokens(key, part):
    row_place = jnp.arange(NH, dtype=jnp.float32) / NH
    col_place = jnp.arange(NW, dtype=jnp.float32) / NW
    low_end, high_end = (math.log(0.6), math.log(1.6))
    region = jnp.exp(jax.random.uniform(jax.random.fold_in(key, 22), (NH // WIN, NW // WIN), jnp.float32, low_end, high_end))
    region = jnp.repeat(jnp.repeat(region, WIN, axis=0), WIN, axis=1)
    pattern = jnp.clip(jax.random.normal(jax.random.fold_in(key, 21), (C,), jnp.float32), -3.0, 3.0)
    noise = jnp.clip(jax.random.normal(jax.random.fold_in(key, 24), (NH, NW, C), jnp.float32), -4.0, 4.0)
    ramp = 0.1 * jnp.power(12.0, row_place)[:, None] * jnp.power(2.5, col_place)[None, :]
    drawn = noise + (ramp * region)[:, :, None] * pattern[None, None, :]
    return jnp.clip(drawn, -8.0, 8.0).astype(jnp.bfloat16)


def scatter_about(own_key, shape, scale, most, held_as=jnp.bfloat16):
    values = scale * jax.random.normal(own_key, shape, jnp.float32)
    return jnp.clip(values, min=-most, max=most).astype(held_as)


def setup_inputs(seed: int = 0) -> dict:
    key_of = jax.random.split(jax.random.key(seed), 12)
    scene_tokens = draw_scene_tokens(jax.random.fold_in(key_of[11], 71), 0)
    block_qkv = draw_block_qkv(jax.random.fold_in(key_of[11], 71), 0)
    block_proj = scatter_about(key_of[2], (3, C, C), C ** -0.5, 0.4375)
    conv_squeeze = scatter_about(key_of[3], (3, 9, C, CC), (9 * C) ** -0.5, 0.15625)
    conv_expand = scatter_about(key_of[4], (3, 9, CC, C), (9 * CC) ** -0.5, 0.25)
    gate_down = scatter_about(key_of[5], (3, C, CS), 1.0, 4.0)
    gate_up = scatter_about(key_of[6], (3, CS, C), 1.0, 6.0)
    mlp_in = scatter_about(key_of[7], (4, C, HID), C ** -0.5, 0.4375)
    mlp_out = scatter_about(key_of[8], (4, HID, C), HID ** -0.5, 0.3125)
    ocab_qkv = draw_ocab_qkv(jax.random.fold_in(key_of[11], 71), 0)
    ocab_proj = scatter_about(key_of[10], (C, C), C ** -0.5, 0.4375)
    return dict(scene_tokens=scene_tokens, block_qkv=block_qkv, block_proj=block_proj, conv_squeeze=conv_squeeze, conv_expand=conv_expand, gate_down=gate_down, gate_up=gate_up, mlp_in=mlp_in, mlp_out=mlp_out, ocab_qkv=ocab_qkv, ocab_proj=ocab_proj)


EPSILON = 1e-05
MASKED = -1000000000.0

def layer_norm(stream):
    middle = lax.optimization_barrier(jnp.mean(stream, axis=-1, keepdims=True))
    centered = stream - middle
    spread = lax.optimization_barrier(jnp.mean(centered * centered, axis=-1, keepdims=True))
    return (centered * lax.rsqrt(spread + EPSILON)).astype(jnp.bfloat16)

def partition(field):
    height, breadth, channels = field.shape
    blocks = field.reshape(height // WIN, WIN, breadth // WIN, WIN, channels)
    return blocks.transpose(0, 2, 1, 3, 4).reshape(height // WIN, breadth // WIN, WIN * WIN, channels)

def assemble(blocks):
    row_count, col_count, window_cells, channels = blocks.shape
    field = blocks.reshape(row_count, col_count, WIN, WIN, channels).transpose(0, 2, 1, 3, 4)
    return field.reshape(row_count * WIN, col_count * WIN, channels)

def attend_windows(queries, keys, values, allowed, proj_weight):
    groups, length, channels = queries.shape
    head_size = channels // HEADS
    split_q = queries.reshape(groups, length, HEADS, head_size).astype(jnp.float32)
    split_k = keys.reshape(groups, keys.shape[1], HEADS, head_size).astype(jnp.float32)
    split_v = values.reshape(groups, values.shape[1], HEADS, head_size).astype(jnp.float32)
    scores = jnp.einsum('gqhd,gkhd->ghqk', split_q, split_k) * head_size ** (-0.5)
    if allowed is not None:
        scores = jnp.where(allowed[:, None], scores, MASKED)
    highest = lax.optimization_barrier(jnp.max(scores, axis=-1, keepdims=True))
    powers = jnp.exp(scores - highest)
    weights = (powers / lax.optimization_barrier(jnp.sum(powers, axis=-1, keepdims=True))).astype(jnp.bfloat16)
    heads_out = jnp.einsum('ghqk,gkhd->gqhd', weights.astype(jnp.float32), split_v).astype(jnp.bfloat16)
    merged = heads_out.reshape(groups * length, channels)
    return jnp.dot(merged, proj_weight, preferred_element_type=jnp.float32).reshape(groups, length, channels)

def rolled_labels(start, number, extent):
    position = start + jnp.arange(number, dtype=jnp.int32)
    return jnp.where(position >= extent - SHIFT, 2, jnp.where(position >= extent - WIN, 1, 0))

def window_branch(normed, qkv_weight, proj_weight, shifted):
    projected = jnp.dot(normed.reshape(NH * NW, C), qkv_weight, preferred_element_type=jnp.float32)
    projected = projected.astype(jnp.bfloat16).reshape(NH, NW, 3 * C)
    if shifted:
        projected = jnp.roll(projected, (-SHIFT, -SHIFT), axis=(0, 1))
    windows = partition(projected)
    column_labels = rolled_labels(0, NW, NW).reshape(NW // WIN, 1, WIN)

    def one_row(pair):
        row_windows, number = pair
        allowed = None
        if shifted:
            row_labels = rolled_labels(number * WIN, WIN, NH)
            labels = (3 * row_labels[None, :, None] + column_labels).reshape(NW // WIN, WIN * WIN)
            allowed = labels[:, :, None] == labels[:, None, :]
        return attend_windows(row_windows[..., :C], row_windows[..., C:2 * C], row_windows[..., 2 * C:], allowed, proj_weight)
    result = assemble(lax.map(one_row, (windows, jnp.arange(NH // WIN, dtype=jnp.int32))))
    if shifted:
        result = jnp.roll(result, (SHIFT, SHIFT), axis=(0, 1))
    return result

def convolve(extended, taps, height, breadth):
    channels_in = extended.shape[2]
    summed = jnp.zeros((height * breadth, taps.shape[2]), jnp.float32)
    for offset in range(9):
        row_step, col_step = (offset // 3, offset % 3)
        window = extended[row_step:row_step + height, col_step:col_step + breadth].reshape(height * breadth, channels_in)
        summed = summed + jnp.dot(window, taps[offset], preferred_element_type=jnp.float32)
    return summed.reshape(height, breadth, taps.shape[2])

def channel_gate(expanded, squeeze_weight, excite_weight):
    pooled = lax.optimization_barrier(jnp.sum(expanded, axis=(0, 1))) / (NH * NW)
    squeezed = jax.nn.relu(jnp.dot(pooled[None], squeeze_weight.astype(jnp.float32), precision=lax.Precision.HIGHEST))
    scaled = jax.nn.sigmoid(jnp.dot(squeezed, excite_weight.astype(jnp.float32), precision=lax.Precision.HIGHEST))
    return expanded * scaled[0]

def feed_forward(normed, in_weight, out_weight):
    height, breadth = (normed.shape[0], normed.shape[1])
    hidden = jax.nn.gelu(jnp.dot(normed.reshape(height * breadth, C), in_weight, preferred_element_type=jnp.float32), approximate=False).astype(jnp.bfloat16)
    return jnp.dot(hidden, out_weight, preferred_element_type=jnp.float32).reshape(height, breadth, C)

def intersection_branch(normed, qkv_weight, proj_weight):
    tokens_flat = normed.reshape(NH * NW, C)
    queries = jnp.dot(tokens_flat, qkv_weight[:, :C], preferred_element_type=jnp.float32).astype(jnp.bfloat16).reshape(NH, NW, C)
    key_values = jnp.dot(tokens_flat, qkv_weight[:, C:], preferred_element_type=jnp.float32).astype(jnp.bfloat16).reshape(NH, NW, 2 * C)
    key_values = jnp.pad(key_values, ((OVL, OVL), (OVL, OVL), (0, 0)))
    context_side = WIN + 2 * OVL
    starts = jnp.arange(NW // WIN, dtype=jnp.int32) * WIN

    def one_row(pair):
        row_queries, number = pair
        band_rows = lax.dynamic_slice_in_dim(key_values, number * WIN, context_side, 0)
        context = jax.vmap(lambda column_start: lax.dynamic_slice_in_dim(band_rows, column_start, context_side, 1))(starts)
        context = context.reshape(NW // WIN, context_side * context_side, 2 * C)
        return attend_windows(row_queries, context[..., :C], context[..., C:], None, proj_weight)
    result = lax.map(one_row, (partition(queries), jnp.arange(NH // WIN, dtype=jnp.int32)))
    return assemble(result)

def reference(scene_tokens, block_qkv, block_proj, conv_squeeze, conv_expand, gate_down, gate_up, mlp_in, mlp_out, ocab_qkv, ocab_proj):
    stream = scene_tokens.astype(jnp.float32)
    edges = ((1, 1), (1, 1), (0, 0))
    for block_number in range(3):
        normed = layer_norm(stream)
        attended = window_branch(normed, block_qkv[block_number], block_proj[block_number], block_number == 1)
        hidden = jax.nn.gelu(convolve(jnp.pad(normed, edges), conv_squeeze[block_number], NH, NW), approximate=False).astype(jnp.bfloat16)
        expanded = convolve(jnp.pad(hidden, edges), conv_expand[block_number], NH, NW)
        gated = channel_gate(expanded, gate_down[block_number], gate_up[block_number])
        stream = stream + attended + gated
        stream = stream + feed_forward(layer_norm(stream), mlp_in[block_number], mlp_out[block_number])
    stream = stream + intersection_branch(layer_norm(stream), ocab_qkv, ocab_proj)
    stream = stream + feed_forward(layer_norm(stream), mlp_in[3], mlp_out[3])
    return stream.astype(jnp.bfloat16)
```

```python
import jax
import jax.numpy as jnp
from jax import lax
from jax.experimental import pallas as pl
from jax.experimental.pallas import tpu as pltpu
from jax.sharding import PartitionSpec as P

C = 180
HEADS = 6
HD = C // HEADS
WIN = 16
L = 256
HID = 360
HL = 384
ROWS = 8
COLS = 16
H = 16
W = 64
E = 80
HALO = (2, 8, 2, 4)
EPSILON = 1e-05
BIG = -1e30
QSCALE = HD ** (-0.5) * 1.4426950408889634
F32 = jnp.float32
BF16 = jnp.bfloat16
MESH = pl.DeviceIdType.MESH


def dot(a, b):
    return jnp.dot(a, b, preferred_element_type=F32)


def dot_t(a, b):
    return lax.dot_general(a, b, (((1,), (1,)), ((), ())), preferred_element_type=F32)


def gelu(v):
    return v * (1.0 + lax.erf(v * 0.7071067811865476)) * 0.5


def iota(shape, dim):
    return lax.broadcasted_iota(jnp.int32, shape, dim)


def layer_norm(x):
    nd = x.ndim
    inside = iota((1,) * (nd - 1) + (L,), nd - 1) < C
    mean = jnp.sum(x, axis=-1, keepdims=True) * (1.0 / C)
    centered = jnp.where(inside, x - mean, 0.0)
    spread = jnp.sum(centered * centered, axis=-1, keepdims=True) * (1.0 / C)
    return centered * lax.rsqrt(spread + EPSILON)


def attend(q, k, v, group):
    tq = q.shape[0]
    lane = iota((1, L), 1)
    total = None
    for first in range(0, HEADS, group):
        stacked = []
        for h in range(first, first + group):
            mask = ((lane >= h * HD) & (lane < h * HD + HD)) | (lane >= C)
            stacked.append(q * mask.astype(F32).astype(BF16))
        qm = jnp.concatenate(stacked, axis=0)
        s = dot_t(qm, k)
        p = jnp.exp2(s - jnp.max(s, axis=-1, keepdims=True))
        inv = 1.0 / jnp.sum(p, axis=-1, keepdims=True)
        r = dot(p.astype(BF16), v) * inv
        for i in range(group):
            h = first + i
            mask = (lane >= h * HD) & (lane < h * HD + HD)
            part = jnp.where(mask, r[i * tq : (i + 1) * tq], 0.0)
            total = part if total is None else total + part
    return total.astype(BF16)


def kernel(
    tok, wqkv, wp, w1, w2, gd, gu, m1, m2, out,
    st, un, ue, rl, rr, qs, ks, vs, qe, ke, ve, att, ex, c1, h32, hc, c2, ara, arb,
    hs, hr, asend, arecv, bsend, brecv,
):
    row = lax.axis_index("row")
    col = lax.axis_index("col")
    up, down = lax.rem(row + ROWS - 1, ROWS), lax.rem(row + 1, ROWS)
    left, right = lax.rem(col + COLS - 1, COLS), lax.rem(col + 1, COLS)

    barrier = pltpu.get_barrier_semaphore()
    peers = [(lax.rem(row + d, ROWS), col) for d in range(1, ROWS)]
    peers += [(row, lax.rem(col + d, COLS)) for d in range(1, COLS)]
    peers += [(up, left), (up, right), (down, left), (down, right)]
    for peer in peers:
        pl.semaphore_signal(barrier, inc=1, device_id=peer, device_id_type=MESH)

    st[...] = jnp.zeros_like(st)
    st[:, :, :C] = tok[...].astype(F32)
    pl.semaphore_wait(barrier, len(peers))

    def remote(src, dst, send, recv, peer):
        return pltpu.make_async_remote_copy(
            src_ref=src, dst_ref=dst, send_sem=send, recv_sem=recv, device_id=peer, device_id_type=MESH
        )

    def halo_copies(k):
        n = HALO[k]
        u, a, b = ue.at[k], rl.at[k], rr.at[k]
        top, low = pl.ds(8, n), pl.ds(24 - n, n)
        above, below = pl.ds(8 - n, n), pl.ds(24, n)
        mid = pl.ds(8, H)
        first, last = pl.ds(0, 16), pl.ds(64, 16)
        plan = [
            (u.at[top], u.at[below], (up, col)),
            (u.at[low], u.at[above], (down, col)),
            (u.at[mid, first], b.at[mid], (row, left)),
            (u.at[mid, last], a.at[mid], (row, right)),
            (u.at[top, first], b.at[below], (up, left)),
            (u.at[top, last], a.at[below], (up, right)),
            (u.at[low, first], b.at[above], (down, left)),
            (u.at[low, last], a.at[above], (down, right)),
        ]
        return [remote(s, d, hs.at[k, i], hr.at[k, i], p) for i, (s, d, p) in enumerate(plan)]

    def normalize(k):
        def step(i, carry):
            x = st[pl.ds(i * 8, 8)]
            u = layer_norm(x)
            un[pl.ds(i * 8, 8)] = u.astype(BF16)
            pad = jnp.zeros((8, 8, L), F32)
            ue[k, pl.ds(8 + i * 8, 8)] = jnp.concatenate([pad, u, pad], axis=1).astype(BF16)
            return carry

        lax.fori_loop(0, 2, step, 0)

    def merge(k):
        n = HALO[k]
        rows = pl.ds(8 - n, H + 2 * n)
        half = iota((1, 16, 1), 1) < 8
        a = rl[k, rows].astype(F32)
        t = ue[k, rows, 0:16].astype(F32)
        ue[k, rows, 0:16] = jnp.where(half, a, t).astype(BF16)
        b = rr[k, rows].astype(F32)
        t = ue[k, rows, 64:80].astype(F32)
        ue[k, rows, 64:80] = jnp.where(half, t, b).astype(BF16)

    def clear_outside(k):
        n = HALO[k]
        rows = pl.ds(8 - n, H + 2 * n)

        @pl.when(row == 0)
        def _():
            ue[k, pl.ds(8 - n, n)] = jnp.zeros((n, E, L), BF16)

        @pl.when(row == ROWS - 1)
        def _():
            ue[k, pl.ds(24, n)] = jnp.zeros((n, E, L), BF16)

        half = iota((1, 16, 1), 1) < 8

        @pl.when(col == 0)
        def _():
            t = ue[k, rows, 0:16].astype(F32)
            ue[k, rows, 0:16] = jnp.where(half, 0.0, t).astype(BF16)

        @pl.when(col == COLS - 1)
        def _():
            t = ue[k, rows, 64:80].astype(F32)
            ue[k, rows, 64:80] = jnp.where(half, t, 0.0).astype(BF16)

    def project(k, which, src, dst, rows, width, chunk, at):
        def step(i, carry):
            x = src[pl.ds(at + i * chunk, chunk)].reshape(chunk * width, L)
            y = dot(x, wqkv[k, which])
            if which == 0:
                y = y * QSCALE
            dst[pl.ds(i * chunk, chunk)] = y.astype(BF16).reshape(chunk, width, L)
            return carry

        lax.fori_loop(0, rows // chunk, step, 0)

    def plain_window(k):
        def step(w, carry):
            cols = pl.ds(pl.multiple_of(w * WIN, WIN), WIN)
            q = qs[:, cols].reshape(WIN * WIN, L)
            kk = ks[:, cols].reshape(WIN * WIN, L)
            vv = vs[:, cols].reshape(WIN * WIN, L)
            o = attend(q, kk, vv, HEADS)
            att[:, cols] = dot(o, wp[k]).reshape(WIN, WIN, L)
            return carry

        return step

    def shifted_window(k):
        lane = iota((1, 1, L), 2)
        qcol = iota((8, WIN, 1), 1) >= 8
        qpat = jnp.where(lane == C, 1.0, 0.0) + jnp.where(
            ((lane == C + 1) & ~qcol) | ((lane == C + 2) & qcol), 1.0, 0.0
        )
        krow = iota((WIN, WIN, 1), 0) >= 8
        kcol = iota((WIN, WIN, 1), 1) >= 8

        def step(i, carry):
            ry = i // 5
            w = i - ry * 5
            cols = pl.ds(pl.multiple_of(w * WIN, WIN), WIN)
            split_row = ((ry == 1) & (row == ROWS - 1)) | ((ry == 0) & (row == 0))
            split_col = ((w == 4) & (col == COLS - 1)) | ((w == 0) & (col == 0))
            brow = jnp.where(split_row, BIG, 0.0)
            bcol = jnp.where(split_col, BIG, 0.0)
            other = jnp.where(ry == 0, 0.0, 1.0)
            krf = jnp.where(krow, 1.0, 0.0)
            differs = krf * other + (1.0 - krf) * (1.0 - other)
            bias = jnp.where(lane == C, differs * brow, 0.0) + jnp.where(
                ((lane == C + 1) & kcol) | ((lane == C + 2) & ~kcol), bcol, 0.0
            )
            q = (qe[pl.ds(ry * 8, 8), cols].astype(F32) + qpat).astype(BF16)
            kk = (ke[pl.ds(ry * WIN, WIN), cols].astype(F32) + bias).astype(BF16)
            vv = ve[pl.ds(ry * WIN, WIN), cols]
            o = attend(
                q.reshape(8 * WIN, L), kk.reshape(WIN * WIN, L), vv.reshape(WIN * WIN, L), HEADS
            )
            att[pl.ds(ry * 8, 8), cols] = dot(o, wp[k]).reshape(8, WIN, L)
            return carry

        return step

    def cross_window(k):
        lane = iota((1, 1, L), 2)
        qpat = jnp.where(lane == C, 1.0, 0.0)
        kcol = iota((1, 32, 1), 1)
        bias = jnp.where((lane == C) & ((kcol < 4) | (kcol >= 28)), BIG, 0.0)

        def step(w, carry):
            cols = pl.ds(pl.multiple_of(w * WIN, WIN), WIN)
            wide = pl.ds(pl.multiple_of(w * WIN, WIN), 32)
            q = (qs[:, cols].astype(F32) + qpat).astype(BF16).reshape(WIN * WIN, L)
            kk = (ke[pl.ds(4, 24), wide].astype(F32) + bias).astype(BF16).reshape(24 * 32, L)
            vv = ve[pl.ds(4, 24), wide].reshape(24 * 32, L)
            o = attend(q, kk, vv, 2)
            att[:, cols] = dot(o, wp[k]).reshape(WIN, WIN, L)
            return carry

        return step

    def conv_in(k):
        hrow = iota((6, E, 1), 0)
        hcol = iota((6, E, 1), 1)
        lane = iota((1, 1, 128), 2)
        low = jnp.where(col == 0, 8, 0)
        high = jnp.where(col == COLS - 1, 72, E)
        rlow = jnp.where(row == 0, 1, 0)
        rhigh = jnp.where(row == ROWS - 1, 17, 18)

        def step(i, carry):
            acc = None
            for a in range(3):
                x = ue[k, pl.ds(6 + a + i * 6, 6)].reshape(6 * E, L)
                y = dot(x, w1[k, a])
                acc = y if acc is None else acc + y
            r = acc.reshape(6, E, L)
            first, second = r[:, :, :128], r[:, :, 128:]
            s = pltpu.roll(first, 1, 1) + pltpu.roll(first, 64, 2) + pltpu.roll(second, E - 1, 1)
            g = gelu(s)
            rr_ = hrow + i * 6
            ok = (rr_ >= rlow) & (rr_ < rhigh) & (hcol >= low) & (hcol < high) & (lane < 60)
            h32[pl.ds(i * 6, 6)] = jnp.where(ok, g, 0.0)
            return carry

        lax.fori_loop(0, 3, step, 0)

    def conv_out(k):
        def step(i, total):
            lead = h32[pl.ds(i * 4, 4)]
            mid = h32[pl.ds(i * 4 + 1, 4)]
            tail = h32[pl.ds(i * 4 + 2, 4)]
            x = jnp.concatenate([lead + pltpu.roll(mid, 64, 2), tail], axis=2)
            x = x.astype(BF16).reshape(4 * E, L)
            r0 = dot(x, w2[k, 0]).reshape(4, E, L)
            r1 = dot(x, w2[k, 1]).reshape(4, E, L)
            r2 = dot(x, w2[k, 2]).reshape(4, E, L)
            y = (pltpu.roll(r0, 1, 1) + r1 + pltpu.roll(r2, E - 1, 1))[:, 8:72]
            ex[pl.ds(i * 4, 4)] = y
            return total + jnp.sum(jnp.sum(y, axis=0), axis=0, keepdims=True)

        return lax.fori_loop(0, 4, step, jnp.zeros((1, L), F32))

    def stage_a(k):
        return [
            remote(ara.at[k, 0], ara.at[k, d], asend.at[k, d], arecv.at[k, d], (lax.rem(row + d, ROWS), col))
            for d in range(1, ROWS)
        ]

    def stage_b(k):
        return [
            remote(arb.at[k, 0], arb.at[k, d], bsend.at[k, d], brecv.at[k, d], (row, lax.rem(col + d, COLS)))
            for d in range(1, COLS)
        ]

    def start(copies):
        for c in copies:
            c.start()

    def finish(copies):
        for c in copies:
            c.wait()

    def between(k, copies):
        finish(copies)
        s = ara[k, 0]
        for d in range(1, ROWS):
            s = s + ara[k, d]
        arb[k, 0] = s
        nxt = stage_b(k)
        start(nxt)
        return nxt

    def gate(k, copies):
        finish(copies)
        s = arb[k, 0]
        for d in range(1, COLS):
            s = s + arb[k, d]
        pooled = s * (1.0 / (ROWS * COLS * H * W))
        squeezed = jnp.sum(gd[k] * pooled, axis=-1, keepdims=True)
        squeezed = jnp.maximum(squeezed, 0.0)
        z = jnp.sum(gu[k] * squeezed, axis=0, keepdims=True)
        return 1.0 / (1.0 + jnp.exp(-z))

    def feed_forward(k, scale, offset):
        def step(i, carry):
            rows = pl.ds(i * 4, 4)
            x = st[rows] + att[rows, offset : offset + W]
            if scale is not None:
                x = x + ex[rows] * scale.reshape(1, 1, L)
            u = layer_norm(x).astype(BF16).reshape(4 * W, L)
            h = gelu(dot(u, m1[k])).astype(BF16)
            st[rows] = x + dot(h, m2[k]).reshape(4, W, L)
            return carry

        lax.fori_loop(0, 4, step, 0)

    for k in range(4):
        normalize(k)
        halos = halo_copies(k)
        start(halos)
        if k == 1:
            finish(halos)
            merge(k)
            project(k, 0, ue.at[k], qe, H, E, 4, 8)
            project(k, 1, ue.at[k], ke, 32, E, 4, 0)
            project(k, 2, ue.at[k], ve, 32, E, 4, 0)
            clear_outside(k)
            conv = True
            windows = shifted_window(k)
            cuts = (0, 0, 5, 10)
            offset = 8
        elif k == 3:
            project(k, 0, un, qs, H, W, 4, 0)
            finish(halos)
            merge(k)
            clear_outside(k)
            project(k, 1, ue.at[k, pl.ds(4, 24)], ke.at[pl.ds(4, 24)], 24, E, 4, 0)
            project(k, 2, ue.at[k, pl.ds(4, 24)], ve.at[pl.ds(4, 24)], 24, E, 4, 0)
            conv = False
            windows = cross_window(k)
            cuts = (0, 4)
            offset = 0
        else:
            project(k, 0, un, qs, H, W, 4, 0)
            project(k, 1, un, ks, H, W, 4, 0)
            project(k, 2, un, vs, H, W, 4, 0)
            conv = True
            windows = plain_window(k)
            cuts = (0, 2, 3, 4)
            offset = 0
        lax.fori_loop(cuts[0], cuts[1], windows, 0)
        scale = None
        if conv:
            if k != 1:
                finish(halos)
                merge(k)
                clear_outside(k)
            conv_in(k)
            ara[k, 0] = conv_out(k)
            copies = stage_a(k)
            start(copies)
            lax.fori_loop(cuts[1], cuts[2], windows, 0)
            copies = between(k, copies)
            lax.fori_loop(cuts[2], cuts[3], windows, 0)
            scale = gate(k, copies)
        feed_forward(k, scale, offset)
    out[...] = st[:, :, :C].astype(BF16)


def pad_to(value, *sizes):
    lead = value.ndim - len(sizes)
    return jnp.pad(
        value, [(0, 0)] * lead + [(0, s - n) for s, n in zip(sizes, value.shape[lead:], strict=True)]
    )


def local(tok, qkv, proj, squeeze, expand, down, up, mlp_in, mlp_out, oqkv, oproj):
    wqkv = jnp.concatenate([qkv, oqkv[None]]).reshape(4, C, 3, C).transpose(0, 2, 1, 3)
    wqkv = pad_to(wqkv, L, L)
    wp = pad_to(jnp.concatenate([proj, oproj[None]]), L, L)
    w1 = pad_to(squeeze.reshape(3, 3, 3, C, 60).transpose(0, 1, 3, 2, 4), 64)
    w1 = pad_to(w1.reshape(3, 3, C, 192), L, L)
    w2 = pad_to(expand.reshape(3, 3, 3, 60, C).transpose(0, 2, 1, 3, 4), 64, L)
    w2 = pad_to(w2.reshape(3, 3, 192, L), L, L)
    gd = pad_to(down.transpose(0, 2, 1).astype(F32), 8, L)
    gu = pad_to(up.astype(F32), 8, L)
    m1 = pad_to(mlp_in, L, HL)
    m2 = pad_to(mlp_out, HL, L)
    vmem = pl.BlockSpec(memory_space=pltpu.VMEM)
    return pl.pallas_call(
        kernel,
        out_shape=jax.ShapeDtypeStruct((H, W, C), BF16),
        in_specs=[vmem] * 9,
        out_specs=vmem,
        scratch_shapes=[
            pltpu.VMEM((H, W, L), F32),
            pltpu.VMEM((H, W, L), BF16),
            pltpu.VMEM((4, 32, E, L), BF16),
            pltpu.VMEM((4, 32, 16, L), BF16),
            pltpu.VMEM((4, 32, 16, L), BF16),
            pltpu.VMEM((H, W, L), BF16),
            pltpu.VMEM((H, W, L), BF16),
            pltpu.VMEM((H, W, L), BF16),
            pltpu.VMEM((H, E, L), BF16),
            pltpu.VMEM((32, E, L), BF16),
            pltpu.VMEM((32, E, L), BF16),
            pltpu.VMEM((H, E, L), F32),
            pltpu.VMEM((H, W, L), F32),
            pltpu.VMEM((8, 128), F32),
            pltpu.VMEM((18, E, 128), F32),
            pltpu.VMEM((8, 128), F32),
            pltpu.VMEM((8, 128), F32),
            pltpu.VMEM((3, ROWS, 1, L), F32),
            pltpu.VMEM((3, COLS, 1, L), F32),
            pltpu.SemaphoreType.DMA((4, 8)),
            pltpu.SemaphoreType.DMA((4, 8)),
            pltpu.SemaphoreType.DMA((3, ROWS)),
            pltpu.SemaphoreType.DMA((3, ROWS)),
            pltpu.SemaphoreType.DMA((3, COLS)),
            pltpu.SemaphoreType.DMA((3, COLS)),
        ],
        compiler_params=pltpu.CompilerParams(
            collective_id=0, has_side_effects=True, vmem_limit_bytes=60 * 1024 * 1024
        ),
        name="blocks",
    )(tok, wqkv, wp, w1, w2, gd, gu, m1, m2)


def solution(mesh):
    placed = (P("row", "col", None),) + (P(),) * 10
    return jax.shard_map(
        local, mesh=mesh, in_specs=placed, out_specs=P("row", "col", None), check_vma=False
    )
```

```python
import jax
import jax.numpy as jnp
from jax import lax
from jax.experimental import pallas as pl
from jax.experimental.pallas import tpu as pltpu
from jax.sharding import PartitionSpec as P

C = 180
HEADS = 6
HD = C // HEADS
WIN = 16
L = 256
HID = 360
HL = 384
ROWS = 8
COLS = 16
H = 16
W = 64
E = 80
EPSILON = 1e-05
BIG = -1e30
QSCALE = HD ** (-0.5) * 1.4426950408889634
F32 = jnp.float32
BF16 = jnp.bfloat16
MESH = pl.DeviceIdType.MESH
GROUPS = ((0, 2, True), (0, 2, True), (2, 6, False), (0, 2, True), (0, 4, True))


def dot(a, b):
    return jnp.dot(a, b, preferred_element_type=F32)


def dot_t(a, b):
    return lax.dot_general(a, b, (((1,), (1,)), ((), ())), preferred_element_type=F32)


def gelu(v):
    return v * (1.0 + lax.erf(v * 0.7071067811865476)) * 0.5


def iota(shape, dim):
    return lax.broadcasted_iota(jnp.int32, shape, dim)


def layer_norm(x):
    nd = x.ndim
    inside = iota((1,) * (nd - 1) + (L,), nd - 1) < C
    mean = jnp.sum(x, axis=-1, keepdims=True) * (1.0 / C)
    centered = jnp.where(inside, x - mean, 0.0)
    spread = jnp.sum(centered * centered, axis=-1, keepdims=True) * (1.0 / C)
    return centered * lax.rsqrt(spread + EPSILON)


def attend(q, k, v, group):
    tq = q.shape[0]
    lane = iota((1, L), 1)
    total = None
    for first in range(0, HEADS, group):
        stacked = []
        for h in range(first, first + group):
            mask = ((lane >= h * HD) & (lane < h * HD + HD)) | (lane >= C)
            stacked.append(q * mask.astype(F32).astype(BF16))
        qm = jnp.concatenate(stacked, axis=0)
        s = dot_t(qm, k)
        p = jnp.exp2(s - jnp.max(s, axis=-1, keepdims=True))
        inv = 1.0 / jnp.sum(p, axis=-1, keepdims=True)
        r = dot(p.astype(BF16), v) * inv
        for i in range(group):
            h = first + i
            mask = (lane >= h * HD) & (lane < h * HD + HD)
            part = jnp.where(mask, r[i * tq : (i + 1) * tq], 0.0)
            total = part if total is None else total + part
    return total.astype(BF16)


def packed(n):
    return n + (n + 1) // 2


def pack(x, ref):
    n = x.shape[0]
    half = (n + 1) // 2
    ref[0:n] = x[:, :, :128].astype(BF16)
    low = x[:half, :, 128:]
    if n > half:
        high = pltpu.roll(x[half:, :, 128:], 64, 2)
        if n < 2 * half:
            high = jnp.concatenate([high, jnp.zeros_like(low[:1])], axis=0)
        low = low + high
    ref[n : n + half] = low.astype(BF16)


def unpack(ref, n):
    half = (n + 1) // 2
    upper = iota((1, 1, 128), 2) < C - 128
    both = ref[n : n + half].astype(F32)
    b = jnp.where(upper, both, 0.0)
    if n > half:
        high = jnp.where(upper, pltpu.roll(both, 64, 2), 0.0)
        b = jnp.concatenate([b, high[: n - half]], axis=0)
    return jnp.concatenate([ref[0:n].astype(F32), b], axis=2)


def fold(x):
    m = x.shape[0] // 2
    return jnp.concatenate([x[:m], x[m:]], axis=1)


def unfold(x):
    return jnp.concatenate([x[:, :8], x[:, 8:]], axis=0)


def kernel(*refs):
    (
        tok, qkv_h, proj_h, sq_h, ex_h, gd_h, gu_h, m1_h, m2_h, oqkv_h, oproj_h, out,
        rqkv, rproj, rsq, rex, rgd, rgu, rm1, rm2, roqkv, roproj,
        wqkv, wp, w1, w2, gd, gu, m1, m2, tmp,
        st, un, ue, ua, qs, ks, vs, qe, ke, ve, att, ex, h32, ara, arb,
    ) = refs[:46]
    bufs = refs[46 : 46 + 6 * len(GROUPS)]
    wsem, hs, hr, asend, arecv, bsend, brecv = refs[46 + 6 * len(GROUPS) :]
    row_s, row_r, col_s, col_r, cor_s, cor_r = (bufs[i :: 6] for i in range(6))
    row = lax.axis_index("row")
    col = lax.axis_index("col")
    up, down = lax.rem(row + ROWS - 1, ROWS), lax.rem(row + 1, ROWS)
    left, right = lax.rem(col + COLS - 1, COLS), lax.rem(col + 1, COLS)

    barrier = pltpu.get_barrier_semaphore()
    peers = [(lax.rem(row + d, ROWS), col) for d in range(1, ROWS)]
    peers += [(row, lax.rem(col + d, COLS)) for d in range(1, COLS)]
    peers += [(up, left), (up, right), (down, left), (down, right)]
    for peer in peers:
        pl.semaphore_signal(barrier, inc=1, device_id=peer, device_id_type=MESH)

    loads = [
        pltpu.make_async_copy(s, d, wsem.at[i])
        for i, (s, d) in enumerate(
            [
                (qkv_h, rqkv), (proj_h, rproj), (sq_h, rsq), (ex_h, rex), (gd_h, rgd),
                (gu_h, rgu), (m1_h, rm1), (m2_h, rm2), (oqkv_h, roqkv), (oproj_h, roproj),
            ]
        )
    ]
    for c in loads:
        c.start()

    def remote(src, dst, send, recv, peer):
        return pltpu.make_async_remote_copy(
            src_ref=src, dst_ref=dst, send_sem=send, recv_sem=recv, device_id=peer, device_id_type=MESH
        )

    def start(copies):
        for c in copies:
            c.start()

    def finish(copies):
        for c in copies:
            c.wait()


    def prepare_attention(k):
        w = rqkv.at[k] if k < 3 else roqkv
        zero = jnp.zeros((L, L), BF16)
        for i in range(3):
            wqkv[k, i] = zero
        whole = w[...]
        wqkv[k, 0, 0:C, 0:C] = w[:, 0:C]
        for i in range(1, 3):
            pick = (iota((3 * C, L), 0) == iota((3 * C, L), 1) + i * C) & (iota((3 * C, L), 1) < C)
            wqkv[k, i, 0:C] = dot(whole, jnp.where(pick, 1.0, 0.0).astype(BF16)).astype(BF16)
        wp[k] = zero
        wp[k, 0:C, 0:C] = rproj[k] if k < 3 else roproj[...]

    def prepare_conv(k):
        zero = jnp.zeros((L, L), BF16)
        for a in range(3):
            w1[k, a] = zero
            tmp[...] = jnp.zeros_like(tmp)
            tmp[0:C, 0:60] = rsq[k, 3 * a + 1].astype(F32)
            w1[k, a, 0:C, 0:60] = rsq[k, 3 * a]
            w1[k, a, 0:C, 128:188] = rsq[k, 3 * a + 2]
            w1[k, a, :, 0:128] = (w1[k, a, :, 0:128].astype(F32) + pltpu.roll(tmp[...], 64, 1)).astype(BF16)
        for b in range(3):
            w2[k, b] = zero
            for a in range(3):
                w2[k, b, 64 * a : 64 * a + 60, 0:C] = rex[k, 3 * a + b]
        tmp[...] = jnp.zeros_like(tmp)
        tmp[0:C, 0:6] = rgd[k].astype(F32)
        gd[k] = tmp[...].T[0:8]
        gu[k] = jnp.zeros((8, L), F32)
        gu[k, 0:6, 0:C] = rgu[k].astype(F32)

    def prepare_mlp(k):
        m1[k] = jnp.zeros((L, HL), BF16)
        m1[k, 0:C, 0:HID] = rm1[k]
        m2[k] = jnp.zeros((HL, L), BF16)
        m2[k, 0:HID, 0:C] = rm2[k]


    def copies_of(g):
        plan = [
            (row_s[g].at[0], row_r[g].at[0], (up, col)),
            (row_s[g].at[1], row_r[g].at[1], (down, col)),
            (col_s[g].at[0], col_r[g].at[0], (row, left)),
            (col_s[g].at[1], col_r[g].at[1], (row, right)),
            (cor_s[g].at[0], cor_r[g].at[0], (up, left)),
            (cor_s[g].at[1], cor_r[g].at[1], (up, right)),
            (cor_s[g].at[2], cor_r[g].at[2], (down, left)),
            (cor_s[g].at[3], cor_r[g].at[3], (down, right)),
        ]
        return [
            remote(s, d, hs.at[g, i], hr.at[g, i], p)
            for i, (s, d, p) in enumerate(plan)
            if GROUPS[g][2] or i not in (2, 3)
        ]

    def send(g):
        d0, n, sides = GROUPS[g]
        top = un[d0 : d0 + n].astype(F32)
        low = un[H - d0 - n : H - d0].astype(F32)
        pack(top, row_s[g].at[0])
        pack(low, row_s[g].at[1])
        pack(fold(top[:, 0:8]), cor_s[g].at[0])
        pack(fold(top[:, W - 8 : W]), cor_s[g].at[1])
        pack(fold(low[:, 0:8]), cor_s[g].at[2])
        pack(fold(low[:, W - 8 : W]), cor_s[g].at[3])
        if sides:
            pack(fold(un[:, 0:16].astype(F32)[:, 0:8]), col_s[g].at[0])
            pack(fold(un[:, W - 16 : W].astype(F32)[:, 8:16]), col_s[g].at[1])
        halos = copies_of(g)
        start(halos)
        return halos

    yes_up = jnp.where(row > 0, 1.0, 0.0)
    yes_down = jnp.where(row < ROWS - 1, 1.0, 0.0)
    yes_left = jnp.where(col > 0, 1.0, 0.0)
    yes_right = jnp.where(col < COLS - 1, 1.0, 0.0)

    def receive(g, masked, whole):
        d0, n, sides = GROUPS[g]
        m = n // 2
        for which, lc, rc, at, keep in ((1, 3, 2, 8 - d0 - n, yes_up), (0, 1, 0, 24 + d0, yes_down)):
            mid = unpack(row_r[g].at[which], n)
            lcorner = unfold(unpack(cor_r[g].at[lc], m))
            rcorner = unfold(unpack(cor_r[g].at[rc], m))
            if whole is not None:
                whole[at : at + n] = jnp.concatenate([lcorner, mid, rcorner], axis=1).astype(BF16)
            if masked is not None:
                masked[at : at + n] = jnp.concatenate(
                    [lcorner * (keep * yes_left), mid * keep, rcorner * (keep * yes_right)], axis=1
                ).astype(BF16)
        if sides:
            lside = unfold(unpack(col_r[g].at[1], 8))
            rside = unfold(unpack(col_r[g].at[0], 8))
            first = un[:, 0:16].astype(F32)[:, 0:8]
            last = un[:, W - 16 : W].astype(F32)[:, 8:16]
            if whole is not None:
                whole[8:24, 0:16] = jnp.concatenate([lside, first], axis=1).astype(BF16)
                whole[8:24, 64:80] = jnp.concatenate([last, rside], axis=1).astype(BF16)
            if masked is not None:
                masked[8:24, 0:16] = jnp.concatenate([lside * yes_left, first], axis=1).astype(BF16)
                masked[8:24, 64:80] = jnp.concatenate([last, rside * yes_right], axis=1).astype(BF16)

    def normalize(k):
        def step(i, carry):
            u = layer_norm(st[pl.ds(i * 8, 8)])
            un[pl.ds(i * 8, 8)] = u.astype(BF16)
            inner = u[:, 8:56].astype(BF16)
            ue[pl.ds(8 + i * 8, 8), 16:64] = inner
            if k == 1:
                ua[pl.ds(8 + i * 8, 8), 16:64] = inner
            return carry

        lax.fori_loop(0, 2, step, 0)

    def project(k, src, targets, first, rows, width, chunk):
        def step(i, carry):
            at = pl.ds(first + i * chunk, chunk)
            x = src[at].reshape(chunk * width, L)
            for which, dst, base in targets:
                y = dot(x, wqkv[k, which])
                if which == 0:
                    y = y * QSCALE
                dst[pl.ds(first - base + i * chunk, chunk)] = y.astype(BF16).reshape(chunk, width, L)
            return carry

        lax.fori_loop(0, rows // chunk, step, 0)


    def plain_window(k):
        def step(w, carry):
            cols = pl.ds(pl.multiple_of(w * WIN, WIN), WIN)
            q = qs[:, cols].reshape(WIN * WIN, L)
            kk = ks[:, cols].reshape(WIN * WIN, L)
            vv = vs[:, cols].reshape(WIN * WIN, L)
            o = attend(q, kk, vv, HEADS)
            att[:, cols] = dot(o, wp[k]).reshape(WIN, WIN, L)
            return carry

        return step

    def shifted_window(k):
        lane = iota((1, 1, L), 2)
        qcol = iota((8, WIN, 1), 1) >= 8
        qpat = jnp.where(lane == C, 1.0, 0.0) + jnp.where(
            ((lane == C + 1) & ~qcol) | ((lane == C + 2) & qcol), 1.0, 0.0
        )
        krow = iota((WIN, WIN, 1), 0) >= 8
        kcol = iota((WIN, WIN, 1), 1) >= 8

        def step(i, carry):
            ry = i // 5
            w = i - ry * 5
            cols = pl.ds(pl.multiple_of(w * WIN, WIN), WIN)
            split_row = ((ry == 1) & (row == ROWS - 1)) | ((ry == 0) & (row == 0))
            split_col = ((w == 4) & (col == COLS - 1)) | ((w == 0) & (col == 0))
            brow = jnp.where(split_row, BIG, 0.0)
            bcol = jnp.where(split_col, BIG, 0.0)
            other = jnp.where(ry == 0, 0.0, 1.0)
            krf = jnp.where(krow, 1.0, 0.0)
            differs = krf * other + (1.0 - krf) * (1.0 - other)
            bias = jnp.where(lane == C, differs * brow, 0.0) + jnp.where(
                ((lane == C + 1) & kcol) | ((lane == C + 2) & ~kcol), bcol, 0.0
            )
            q = (qe[pl.ds(ry * 8, 8), cols].astype(F32) + qpat).astype(BF16)
            kk = (ke[pl.ds(ry * WIN, WIN), cols].astype(F32) + bias).astype(BF16)
            vv = ve[pl.ds(ry * WIN, WIN), cols]
            o = attend(
                q.reshape(8 * WIN, L), kk.reshape(WIN * WIN, L), vv.reshape(WIN * WIN, L), HEADS
            )
            att[pl.ds(ry * 8, 8), cols] = dot(o, wp[k]).reshape(8, WIN, L)
            return carry

        return step

    def cross_window(k):
        lane = iota((1, 1, L), 2)
        qpat = jnp.where(lane == C, 1.0, 0.0)
        kcol = iota((1, 32, 1), 1)
        bias = jnp.where((lane == C) & ((kcol < 4) | (kcol >= 28)), BIG, 0.0)

        def step(w, carry):
            cols = pl.ds(pl.multiple_of(w * WIN, WIN), WIN)
            wide = pl.ds(pl.multiple_of(w * WIN, WIN), 32)
            q = (qs[:, cols].astype(F32) + qpat).astype(BF16).reshape(WIN * WIN, L)
            kk = (ke[pl.ds(4, 24), wide].astype(F32) + bias).astype(BF16).reshape(24 * 32, L)
            vv = ve[pl.ds(4, 24), wide].reshape(24 * 32, L)
            o = attend(q, kk, vv, 2)
            att[:, cols] = dot(o, wp[k]).reshape(WIN, WIN, L)
            return carry

        return step


    def conv_in(k):
        chunk = 9
        hrow = iota((chunk, E, 1), 0)
        hcol = iota((chunk, E, 1), 1)
        lane = iota((1, 1, 128), 2)
        low = jnp.where(col == 0, 8, 0)
        high = jnp.where(col == COLS - 1, 72, E)
        rlow = jnp.where(row == 0, 1, 0)
        rhigh = jnp.where(row == ROWS - 1, 17, 18)

        def step(i, carry):
            acc = None
            for a in range(3):
                x = ue[pl.ds(6 + a + i * chunk, chunk)].reshape(chunk * E, L)
                y = dot(x, w1[k, a])
                acc = y if acc is None else acc + y
            r = acc.reshape(chunk, E, L)
            first, second = r[:, :, :128], r[:, :, 128:]
            s = pltpu.roll(first, 1, 1) + pltpu.roll(first, 64, 2) + pltpu.roll(second, E - 1, 1)
            g = gelu(s)
            at = hrow + i * chunk
            ok = (at >= rlow) & (at < rhigh) & (hcol >= low) & (hcol < high) & (lane < 60)
            h32[pl.ds(i * chunk, chunk)] = jnp.where(ok, g, 0.0)
            return carry

        lax.fori_loop(0, 18 // chunk, step, 0)

    def conv_out(k):
        chunk = 8

        def step(i, total):
            lead = h32[pl.ds(i * chunk, chunk)]
            mid = h32[pl.ds(i * chunk + 1, chunk)]
            tail = h32[pl.ds(i * chunk + 2, chunk)]
            x = jnp.concatenate([lead + pltpu.roll(mid, 64, 2), tail], axis=2)
            x = x.astype(BF16).reshape(chunk * E, L)
            r0 = dot(x, w2[k, 0]).reshape(chunk, E, L)
            r1 = dot(x, w2[k, 1]).reshape(chunk, E, L)
            r2 = dot(x, w2[k, 2]).reshape(chunk, E, L)
            y = (pltpu.roll(r0, 1, 1) + r1 + pltpu.roll(r2, E - 1, 1))[:, 8:72]
            ex[pl.ds(i * chunk, chunk)] = y
            return total + jnp.sum(jnp.sum(y, axis=0), axis=0, keepdims=True)

        return lax.fori_loop(0, H // chunk, step, jnp.zeros((1, L), F32))


    def stage_a(k):
        return [
            remote(ara.at[k, 0], ara.at[k, d], asend.at[k, d], arecv.at[k, d], (lax.rem(row + d, ROWS), col))
            for d in range(1, ROWS)
        ]

    def stage_b(k):
        return [
            remote(arb.at[k, 0], arb.at[k, d], bsend.at[k, d], brecv.at[k, d], (row, lax.rem(col + d, COLS)))
            for d in range(1, COLS)
        ]

    def between(k, copies):
        finish(copies)
        s = ara[k, 0]
        for d in range(1, ROWS):
            s = s + ara[k, d]
        arb[k, 0] = s
        nxt = stage_b(k)
        start(nxt)
        return nxt

    def gate(k, copies):
        finish(copies)
        s = arb[k, 0]
        for d in range(1, COLS):
            s = s + arb[k, d]
        pooled = s * (1.0 / (ROWS * COLS * H * W))
        squeezed = jnp.sum(gd[k] * pooled, axis=-1, keepdims=True)
        squeezed = jnp.maximum(squeezed, 0.0)
        z = jnp.sum(gu[k] * squeezed, axis=0, keepdims=True)
        return 1.0 / (1.0 + jnp.exp(-z))

    def feed_forward(k, scale, offset):
        chunk = 8

        def step(i, carry):
            rows = pl.ds(i * chunk, chunk)
            x = st[rows] + att[rows, offset : offset + W]
            if scale is not None:
                x = x + ex[rows] * scale.reshape(1, 1, L)
            u = layer_norm(x).astype(BF16).reshape(chunk * W, L)
            h = gelu(dot(u, m1[k])).astype(BF16)
            st[rows] = x + dot(h, m2[k]).reshape(chunk, W, L)
            return carry

        lax.fori_loop(0, H // chunk, step, 0)

    st[...] = jnp.zeros_like(st)
    st[:, :, :C] = tok[...].astype(F32)

    normalize(0)
    pl.semaphore_wait(barrier, len(peers))
    halos = send(0)
    finish(loads)
    prepare_attention(0)
    prepare_conv(0)
    project(0, un, ((0, qs, 0), (1, ks, 0), (2, vs, 0)), 0, H, W, 8)
    lax.fori_loop(0, 1, plain_window(0), 0)
    finish(halos)
    receive(0, ue, None)
    conv_in(0)
    ara[0, 0] = conv_out(0)
    copies = stage_a(0)
    start(copies)
    lax.fori_loop(1, 4, plain_window(0), 0)
    copies = between(0, copies)
    for k in range(4):
        prepare_mlp(k)
    for k in range(1, 4):
        prepare_attention(k)
    for k in range(1, 3):
        prepare_conv(k)
    feed_forward(0, gate(0, copies), 0)

    normalize(1)
    halos = send(1)
    more = send(2)
    finish(halos)
    receive(1, ue, ua)
    conv_in(1)
    ara[1, 0] = conv_out(1)
    copies = stage_a(1)
    start(copies)
    project(1, ua, ((0, qe, 8), (1, ke, 0), (2, ve, 0)), 8, H, E, 4)
    copies = between(1, copies)
    finish(more)
    receive(2, None, ua)
    project(1, ua, ((1, ke, 0), (2, ve, 0)), 0, 8, E, 4)
    project(1, ua, ((1, ke, 0), (2, ve, 0)), 24, 8, E, 4)
    lax.fori_loop(0, 10, shifted_window(1), 0)
    feed_forward(1, gate(1, copies), 8)

    normalize(2)
    halos = send(3)
    project(2, un, ((0, qs, 0), (1, ks, 0), (2, vs, 0)), 0, H, W, 8)
    lax.fori_loop(0, 2, plain_window(2), 0)
    finish(halos)
    receive(3, ue, None)
    conv_in(2)
    ara[2, 0] = conv_out(2)
    copies = stage_a(2)
    start(copies)
    lax.fori_loop(2, 4, plain_window(2), 0)
    copies = between(2, copies)
    feed_forward(2, gate(2, copies), 0)

    normalize(3)
    halos = send(4)
    project(3, un, ((0, qs, 0),), 0, H, W, 8)
    finish(halos)
    receive(4, ue, None)
    project(3, ue, ((1, ke, 0), (2, ve, 0)), 4, 24, E, 6)
    lax.fori_loop(0, 4, cross_window(3), 0)
    feed_forward(3, None, 0)
    out[...] = st[:, :, :C].astype(BF16)


def local(*args):
    vmem = pl.BlockSpec(memory_space=pltpu.VMEM)
    hbm = pl.BlockSpec(memory_space=pltpu.HBM)
    scratch = [pltpu.VMEM(a.shape, a.dtype) for a in args[1:]]
    scratch += [
        pltpu.VMEM((4, 3, L, L), BF16),
        pltpu.VMEM((4, L, L), BF16),
        pltpu.VMEM((3, 3, L, L), BF16),
        pltpu.VMEM((3, 3, L, L), BF16),
        pltpu.VMEM((3, 8, L), F32),
        pltpu.VMEM((3, 8, L), F32),
        pltpu.VMEM((4, L, HL), BF16),
        pltpu.VMEM((4, HL, L), BF16),
        pltpu.VMEM((L, 128), F32),
        pltpu.VMEM((H, W, L), F32),
        pltpu.VMEM((H, W, L), BF16),
        pltpu.VMEM((32, E, L), BF16),
        pltpu.VMEM((32, E, L), BF16),
        pltpu.VMEM((H, W, L), BF16),
        pltpu.VMEM((H, W, L), BF16),
        pltpu.VMEM((H, W, L), BF16),
        pltpu.VMEM((H, E, L), BF16),
        pltpu.VMEM((32, E, L), BF16),
        pltpu.VMEM((32, E, L), BF16),
        pltpu.VMEM((H, E, L), F32),
        pltpu.VMEM((H, W, L), F32),
        pltpu.VMEM((18, E, 128), F32),
        pltpu.VMEM((3, ROWS, 1, L), F32),
        pltpu.VMEM((3, COLS, 1, L), F32),
    ]
    for _, n, _ in GROUPS:
        for shape in ((2, packed(n), W, 128), (2, packed(8), 16, 128), (4, packed(n // 2), 16, 128)):
            scratch += [pltpu.VMEM(shape, BF16)] * 2
    dma = pltpu.SemaphoreType.DMA
    scratch += [dma((10,)), dma((len(GROUPS), 8)), dma((len(GROUPS), 8))]
    scratch += [dma((3, ROWS)), dma((3, ROWS)), dma((3, COLS)), dma((3, COLS))]
    return pl.pallas_call(
        kernel,
        out_shape=jax.ShapeDtypeStruct((H, W, C), BF16),
        in_specs=[vmem] + [hbm] * 10,
        out_specs=vmem,
        scratch_shapes=scratch,
        compiler_params=pltpu.CompilerParams(
            collective_id=0, has_side_effects=True, vmem_limit_bytes=60 * 1024 * 1024
        ),
        name="blocks",
    )(*args)


def solution(mesh):
    placed = (P("row", "col", None),) + (P(),) * 10
    return jax.shard_map(
        local, mesh=mesh, in_specs=placed, out_specs=P("row", "col", None), check_vma=False
    )
```

```python
import jax
import jax.numpy as jnp
from jax import lax
from jax.experimental import pallas as pl
from jax.experimental.pallas import tpu as pltpu
from jax.sharding import PartitionSpec as P

C = 180
HEADS = 6
HD = C // HEADS
WIN = 16
L = 256
HID = 360
HL = 384
ROWS = 8
COLS = 16
H = 16
W = 64
E = 80
EPSILON = 1e-05
BIG = -1e30
QSCALE = HD ** (-0.5) * 1.4426950408889634
F32 = jnp.float32
BF16 = jnp.bfloat16
MESH = pl.DeviceIdType.MESH
GROUPS = ((0, 2, True), (0, 2, True), (2, 6, False), (0, 2, True), (0, 4, True))


def dot(a, b):
    return jnp.dot(a, b, preferred_element_type=F32)


def dot_t(a, b):
    return lax.dot_general(a, b, (((1,), (1,)), ((), ())), preferred_element_type=F32)


def gelu(v):
    return v * (1.0 + lax.erf(v * 0.7071067811865476)) * 0.5


def iota(shape, dim):
    return lax.broadcasted_iota(jnp.int32, shape, dim)


def layer_norm(x):
    nd = x.ndim
    inside = iota((1,) * (nd - 1) + (L,), nd - 1) < C
    mean = jnp.sum(x, axis=-1, keepdims=True) * (1.0 / C)
    centered = jnp.where(inside, x - mean, 0.0)
    spread = jnp.sum(centered * centered, axis=-1, keepdims=True) * (1.0 / C)
    return centered * lax.rsqrt(spread + EPSILON)


def attend_part(q, k, v, group):
    tq = q.shape[0]
    lane = iota((1, L), 1)
    num = top = den = None
    for first in range(0, HEADS, group):
        stacked = []
        for h in range(first, first + group):
            mask = ((lane >= h * HD) & (lane < h * HD + HD)) | (lane >= C)
            stacked.append(q * mask.astype(F32).astype(BF16))
        s = dot_t(jnp.concatenate(stacked, axis=0), k)
        m = jnp.max(s, axis=-1, keepdims=True)
        p = jnp.exp2(s - m)
        d = jnp.sum(p, axis=-1, keepdims=True)
        r = dot(p.astype(BF16), v)
        for i in range(group):
            span = slice(i * tq, (i + 1) * tq)
            here = lane >= (first + i) * HD
            wide = [r[span], jnp.broadcast_to(m[span], (tq, L)), jnp.broadcast_to(d[span], (tq, L))]
            if num is None:
                num, top, den = wide
            else:
                num, top, den = (jnp.where(here, x, y) for x, y in zip(wide, (num, top, den)))
    return num, top, den


def attend(q, k, v, group):
    num, _, den = attend_part(q, k, v, group)
    return (num / den).astype(BF16)


def merge_parts(a, b):
    (n0, m0, d0), (n1, m1, d1) = a, b
    m = jnp.maximum(m0, m1)
    c0, c1 = jnp.exp2(m0 - m), jnp.exp2(m1 - m)
    return ((n0 * c0 + n1 * c1) / (d0 * c0 + d1 * c1)).astype(BF16)


def packed(n):
    return n + (n + 1) // 2


def pack(x, ref):
    n = x.shape[0]
    half = (n + 1) // 2
    ref[0:n] = x[:, :, :128].astype(BF16)
    low = x[:half, :, 128:]
    if n > half:
        high = pltpu.roll(x[half:, :, 128:], 64, 2)
        if n < 2 * half:
            high = jnp.concatenate([high, jnp.zeros_like(low[:1])], axis=0)
        low = low + high
    ref[n : n + half] = low.astype(BF16)


def unpack(ref, n):
    half = (n + 1) // 2
    upper = iota((1, 1, 128), 2) < C - 128
    both = ref[n : n + half].astype(F32)
    b = jnp.where(upper, both, 0.0)
    if n > half:
        high = jnp.where(upper, pltpu.roll(both, 64, 2), 0.0)
        b = jnp.concatenate([b, high[: n - half]], axis=0)
    return jnp.concatenate([ref[0:n].astype(F32), b], axis=2)


def fold(x):
    m = x.shape[0] // 2
    return jnp.concatenate([x[:m], x[m:]], axis=1)


def unfold(x):
    return jnp.concatenate([x[:, :8], x[:, 8:]], axis=0)


def kernel(*refs):
    (
        tok, qkv_h, proj_h, sq_h, ex_h, gd_h, gu_h, m1_h, m2_h, oqkv_h, oproj_h, out,
        rqkv, rproj, rsq, rex, rgd, rgu, rm1, rm2, roqkv, roproj,
        wqkv, wp, w1, w2, gd, gu, m1, m2, tmp, pn, pm, pd,
        st, un, ue, ua, qs, ks, vs, qe, ke, ve, att, ex, h32, ara, arb,
    ) = refs[:49]
    bufs = refs[49 : 49 + 6 * len(GROUPS)]
    wsem, hs, hr, asend, arecv, bsend, brecv = refs[49 + 6 * len(GROUPS) :]
    row_s, row_r, col_s, col_r, cor_s, cor_r = (bufs[i :: 6] for i in range(6))
    row = lax.axis_index("row")
    col = lax.axis_index("col")
    up, down = lax.rem(row + ROWS - 1, ROWS), lax.rem(row + 1, ROWS)
    left, right = lax.rem(col + COLS - 1, COLS), lax.rem(col + 1, COLS)

    barrier = pltpu.get_barrier_semaphore()
    peers = [(lax.rem(row + d, ROWS), col) for d in range(1, ROWS)]
    peers += [(row, lax.rem(col + d, COLS)) for d in range(1, COLS)]
    peers += [(up, left), (up, right), (down, left), (down, right)]
    for peer in peers:
        pl.semaphore_signal(barrier, inc=1, device_id=peer, device_id_type=MESH)

    loads = [
        pltpu.make_async_copy(s, d, wsem.at[i])
        for i, (s, d) in enumerate(
            [
                (qkv_h, rqkv), (proj_h, rproj), (sq_h, rsq), (ex_h, rex), (gd_h, rgd),
                (gu_h, rgu), (m1_h, rm1), (m2_h, rm2), (oqkv_h, roqkv), (oproj_h, roproj),
            ]
        )
    ]
    for c in loads:
        c.start()

    def remote(src, dst, send, recv, peer):
        return pltpu.make_async_remote_copy(
            src_ref=src, dst_ref=dst, send_sem=send, recv_sem=recv, device_id=peer, device_id_type=MESH
        )

    def start(copies):
        for c in copies:
            c.start()

    def finish(copies):
        for c in copies:
            c.wait()


    def prepare_attention(k):
        w = rqkv.at[k] if k < 3 else roqkv
        zero = jnp.zeros((L, L), BF16)
        for i in range(3):
            wqkv[k, i] = zero
        whole = w[...]
        wqkv[k, 0, 0:C, 0:C] = w[:, 0:C]
        for i in range(1, 3):
            pick = (iota((3 * C, L), 0) == iota((3 * C, L), 1) + i * C) & (iota((3 * C, L), 1) < C)
            wqkv[k, i, 0:C] = dot(whole, jnp.where(pick, 1.0, 0.0).astype(BF16)).astype(BF16)
        wp[k] = zero
        wp[k, 0:C, 0:C] = rproj[k] if k < 3 else roproj[...]

    def prepare_conv(k):
        zero = jnp.zeros((L, L), BF16)
        for a in range(3):
            tmp[:, 0:L] = zero
            for b in range(3):
                tmp[64 * b : 64 * b + 60, 0:C] = rsq[k, 3 * a + b]
            w1[k, a] = tmp[:, 0:L].astype(F32).T.astype(BF16)
        for b in range(3):
            w2[k, b] = zero
            for a in range(3):
                w2[k, b, 64 * a : 64 * a + 60, 0:C] = rex[k, 3 * a + b]
        for dst, raw in ((gd, rgd), (gu, rgu)):
            dst[k] = jnp.zeros((8, L), F32)
            dst[k, 0:6, 0:C] = raw[k].astype(F32)

    def prepare_mlp(k):
        m1[k] = jnp.zeros((L, HL), BF16)
        m1[k, 0:C, 0:HID] = rm1[:, k, :]
        tmp[...] = jnp.zeros((L, HL), BF16)
        tmp[0:C, 0:HID] = rm2[:, k, :]
        m2[k] = tmp[...].astype(F32).T.astype(BF16)


    def copies_of(g, which):
        plan = [
            (row_s[g].at[0], row_r[g].at[0], (up, col)),
            (row_s[g].at[1], row_r[g].at[1], (down, col)),
            (col_s[g].at[0], col_r[g].at[0], (row, left)),
            (col_s[g].at[1], col_r[g].at[1], (row, right)),
            (cor_s[g].at[0], cor_r[g].at[0], (up, left)),
            (cor_s[g].at[1], cor_r[g].at[1], (up, right)),
            (cor_s[g].at[2], cor_r[g].at[2], (down, left)),
            (cor_s[g].at[3], cor_r[g].at[3], (down, right)),
        ]
        return [
            remote(s, d, hs.at[g, i], hr.at[g, i], p)
            for i, (s, d, p) in enumerate(plan)
            if i in which
        ]

    def send_rows(g):
        d0, n, _ = GROUPS[g]
        top = un[d0 : d0 + n].astype(F32)
        low = un[H - d0 - n : H - d0].astype(F32)
        pack(top, row_s[g].at[0])
        pack(low, row_s[g].at[1])
        pack(fold(top[:, 0:8]), cor_s[g].at[0])
        pack(fold(top[:, W - 8 : W]), cor_s[g].at[1])
        pack(fold(low[:, 0:8]), cor_s[g].at[2])
        pack(fold(low[:, W - 8 : W]), cor_s[g].at[3])
        rows = copies_of(g, (0, 1, 4, 5, 6, 7))
        start(rows)
        return rows

    def send_sides(g):
        pack(fold(un[:, 0:16].astype(F32)[:, 0:8]), col_s[g].at[0])
        pack(fold(un[:, W - 16 : W].astype(F32)[:, 8:16]), col_s[g].at[1])
        sides = copies_of(g, (2, 3))
        start(sides)
        return sides

    yes_up = jnp.where(row > 0, 1.0, 0.0)
    yes_down = jnp.where(row < ROWS - 1, 1.0, 0.0)
    yes_left = jnp.where(col > 0, 1.0, 0.0)
    yes_right = jnp.where(col < COLS - 1, 1.0, 0.0)

    def receive_rows(g, masked, whole):
        d0, n, _ = GROUPS[g]
        m = n // 2
        for which, lc, rc, at, keep in ((1, 3, 2, 8 - d0 - n, yes_up), (0, 1, 0, 24 + d0, yes_down)):
            mid = unpack(row_r[g].at[which], n)
            lcorner = unfold(unpack(cor_r[g].at[lc], m))
            rcorner = unfold(unpack(cor_r[g].at[rc], m))
            if whole is not None:
                whole[at : at + n] = jnp.concatenate([lcorner, mid, rcorner], axis=1).astype(BF16)
            if masked is not None:
                masked[at : at + n] = jnp.concatenate(
                    [lcorner * (keep * yes_left), mid * keep, rcorner * (keep * yes_right)], axis=1
                ).astype(BF16)

    def receive_sides(g, masked, whole):
        lside = unfold(unpack(col_r[g].at[1], 8))
        rside = unfold(unpack(col_r[g].at[0], 8))
        first = un[:, 0:16].astype(F32)[:, 0:8]
        last = un[:, W - 16 : W].astype(F32)[:, 8:16]
        if whole is not None:
            whole[8:24, 0:16] = jnp.concatenate([lside, first], axis=1).astype(BF16)
            whole[8:24, 64:80] = jnp.concatenate([last, rside], axis=1).astype(BF16)
        if masked is not None:
            masked[8:24, 0:16] = jnp.concatenate([lside * yes_left, first], axis=1).astype(BF16)
            masked[8:24, 64:80] = jnp.concatenate([last, rside * yes_right], axis=1).astype(BF16)

    def normalize(k, y, rows):
        u = layer_norm(y)
        un[rows] = u.astype(BF16)
        inner = u[:, 8:56].astype(BF16)
        at = pl.ds(rows.start + 8, rows.size)
        ue[at, 16:64] = inner
        if k == 1:
            ua[at, 16:64] = inner

    def project(k, which, x):
        r, c, _ = x.shape
        y = dot(x.reshape(r * c, L), wqkv[k, which])
        if which == 0:
            y = y * QSCALE
        return y.astype(BF16).reshape(r, c, L)

    def project_plain(k, dsts):
        def step(i, carry):
            rows = pl.ds(i * 8, 8)
            x = un[rows]
            for which, dst in enumerate(dsts):
                dst[rows] = project(k, which, x)
            return carry

        lax.fori_loop(0, 2, step, 0)

    def project_inner(k, src, dsts):
        def step(i, carry):
            x = src[pl.ds(8 + 8 * i, 8), 16:64]
            for which, dst, base in dsts:
                dst[pl.ds(8 - base + 8 * i, 8), 16:64] = project(k, which, x)
            return carry

        lax.fori_loop(0, 2, step, 0)

    def project_sides(k, src, dsts):
        x = jnp.concatenate([src[8:24, 0:16], src[8:24, 64:80]], axis=1)
        for which, dst, base in dsts:
            y = project(k, which, x)
            dst[8 - base : 24 - base, 0:16] = y[:, 0:16]
            dst[8 - base : 24 - base, 64:80] = y[:, 16:32]

    def project_rows(k, src, n):
        for at in (8 - n, 24):
            x = src[at : at + n]
            for which, dst in ((1, ke), (2, ve)):
                dst[at : at + n] = project(k, which, x)


    def plain_window(k):
        def step(w, carry):
            cols = pl.ds(pl.multiple_of(w * WIN, WIN), WIN)
            q = qs[:, cols].reshape(WIN * WIN, L)
            kk = ks[:, cols].reshape(WIN * WIN, L)
            vv = vs[:, cols].reshape(WIN * WIN, L)
            o = attend(q, kk, vv, HEADS)
            att[:, cols] = dot(o, wp[k]).reshape(WIN, WIN, L)
            return carry

        return step

    def keep_part(at, part):
        for ref, value in zip((pn, pm, pd), part):
            ref[at] = value.reshape(at.size, 128, L)

    def kept_part(at):
        return tuple(ref[at].reshape(at.size * 128, L) for ref in (pn, pm, pd))

    def shifted_part(k, ry, w, near):
        lane = iota((1, 1, L), 2)
        qcol = iota((8, WIN, 1), 1) >= 8
        qpat = jnp.where(lane == C, 1.0, 0.0) + jnp.where(
            ((lane == C + 1) & ~qcol) | ((lane == C + 2) & qcol), 1.0, 0.0
        )
        kcol = iota((8, WIN, 1), 1) >= 8
        cols = pl.ds(pl.multiple_of(w * WIN, WIN), WIN)
        split_row = ((ry == 1) & (row == ROWS - 1)) | ((ry == 0) & (row == 0))
        split_col = ((w == 4) & (col == COLS - 1)) | ((w == 0) & (col == 0))
        bcol = jnp.where(split_col, BIG, 0.0)
        bias = jnp.where(((lane == C + 1) & kcol) | ((lane == C + 2) & ~kcol), bcol, 0.0)
        if near:
            rows = pl.ds(8 + ry * 8, 8)
        else:
            rows = pl.ds(ry * 24, 8)
            bias = bias + jnp.where(lane == C, jnp.where(split_row, BIG, 0.0), 0.0)
        q = (qe[pl.ds(ry * 8, 8), cols].astype(F32) + qpat).astype(BF16).reshape(8 * WIN, L)
        kk = (ke[rows, cols].astype(F32) + bias).astype(BF16).reshape(8 * WIN, L)
        vv = ve[rows, cols].reshape(8 * WIN, L)
        return attend_part(q, kk, vv, HEADS)

    def shifted_near(k, count, width, first, stride):
        def step(i, carry):
            ry = i // width
            w = first + stride * (i - ry * width)
            keep_part(pl.ds(ry * 5 + w, 1), shifted_part(k, ry, w, True))
            return carry

        lax.fori_loop(0, count, step, 0)

    def shifted_far(k):
        def step(i, carry):
            ry = i // 5
            w = i - ry * 5
            cols = pl.ds(pl.multiple_of(w * WIN, WIN), WIN)
            o = merge_parts(kept_part(pl.ds(i, 1)), shifted_part(k, ry, w, False))
            att[pl.ds(ry * 8, 8), cols] = dot(o, wp[k]).reshape(8, WIN, L)
            return carry

        return step

    def cross_part(k, w, rows):
        lane = iota((1, 1, L), 2)
        qpat = jnp.where(lane == C, 1.0, 0.0)
        kcol = iota((1, 32, 1), 1)
        bias = jnp.where((lane == C) & ((kcol < 4) | (kcol >= 28)), BIG, 0.0)
        cols = pl.ds(pl.multiple_of(w * WIN, WIN), WIN)
        wide = pl.ds(pl.multiple_of(w * WIN, WIN), 32)
        q = (qs[:, cols].astype(F32) + qpat).astype(BF16).reshape(WIN * WIN, L)
        kk = jnp.concatenate([ke[r, wide] for r in rows], axis=0)
        vv = jnp.concatenate([ve[r, wide] for r in rows], axis=0)
        n = kk.shape[0] * 32
        kk = (kk.astype(F32) + bias).astype(BF16).reshape(n, L)
        return attend_part(q, kk, vv.reshape(n, L), 2)

    def cross_near(k, first, stride):
        def step(i, carry):
            w = first + stride * i
            keep_part(pl.ds(2 * w, 2), cross_part(k, w, (pl.ds(8, 16),)))
            return carry

        lax.fori_loop(0, 2, step, 0)

    def cross_far(k):
        def step(w, carry):
            cols = pl.ds(pl.multiple_of(w * WIN, WIN), WIN)
            far = cross_part(k, w, (pl.ds(4, 4), pl.ds(24, 4)))
            o = merge_parts(kept_part(pl.ds(2 * w, 2)), far)
            att[:, cols] = dot(o, wp[k]).reshape(WIN, WIN, L)
            return carry

        return step


    def conv_in(k):
        chunk = 9
        hrow = iota((chunk, E, 1), 0)
        hcol = iota((chunk, E, 1), 1)
        lane = iota((1, 1, 128), 2)
        low = jnp.where(col == 0, 8, 0)
        high = jnp.where(col == COLS - 1, 72, E)
        rlow = jnp.where(row == 0, 1, 0)
        rhigh = jnp.where(row == ROWS - 1, 17, 18)

        def step(i, carry):
            acc = None
            for a in range(3):
                x = ue[pl.ds(6 + a + i * chunk, chunk)].reshape(chunk * E, L)
                y = dot(x, w1[k, a])
                acc = y if acc is None else acc + y
            r = acc.reshape(chunk, E, L)
            first, second = r[:, :, :128], r[:, :, 128:]
            s = pltpu.roll(first, 1, 1) + pltpu.roll(first, 64, 2) + pltpu.roll(second, E - 1, 1)
            g = gelu(s)
            at = hrow + i * chunk
            ok = (at >= rlow) & (at < rhigh) & (hcol >= low) & (hcol < high) & (lane < 60)
            h32[pl.ds(i * chunk, chunk)] = jnp.where(ok, g, 0.0)
            return carry

        lax.fori_loop(0, 18 // chunk, step, 0)

    def conv_out(k):
        chunk = 8

        def step(i, total):
            lead = h32[pl.ds(i * chunk, chunk)]
            mid = h32[pl.ds(i * chunk + 1, chunk)]
            tail = h32[pl.ds(i * chunk + 2, chunk)]
            x = jnp.concatenate([lead + pltpu.roll(mid, 64, 2), tail], axis=2)
            x = x.astype(BF16).reshape(chunk * E, L)
            r0 = dot(x, w2[k, 0]).reshape(chunk, E, L)
            r1 = dot(x, w2[k, 1]).reshape(chunk, E, L)
            r2 = dot(x, w2[k, 2]).reshape(chunk, E, L)
            y = (pltpu.roll(r0, 1, 1) + r1 + pltpu.roll(r2, E - 1, 1))[:, 8:72]
            ex[pl.ds(i * chunk, chunk)] = y
            return total + jnp.sum(jnp.sum(y, axis=0), axis=0, keepdims=True)

        return lax.fori_loop(0, H // chunk, step, jnp.zeros((1, L), F32))


    def stage_a(k):
        return [
            remote(ara.at[k, 0], ara.at[k, d], asend.at[k, d], arecv.at[k, d], (lax.rem(row + d, ROWS), col))
            for d in range(1, ROWS)
        ]

    def stage_b(k):
        return [
            remote(arb.at[k, 0], arb.at[k, d], bsend.at[k, d], brecv.at[k, d], (row, lax.rem(col + d, COLS)))
            for d in range(1, COLS)
        ]

    def between(k, copies):
        finish(copies)
        s = ara[k, 0]
        for d in range(1, ROWS):
            s = s + ara[k, d]
        arb[k, 0] = s
        nxt = stage_b(k)
        start(nxt)
        return nxt

    def gate(k, copies):
        finish(copies)
        s = arb[k, 0]
        for d in range(1, COLS):
            s = s + arb[k, d]
        pooled = s * (1.0 / (ROWS * COLS * H * W))
        squeezed = jnp.sum(gd[k] * pooled, axis=-1, keepdims=True)
        squeezed = jnp.maximum(squeezed, 0.0)
        z = jnp.sum(gu[k] * squeezed, axis=0, keepdims=True)
        return 1.0 / (1.0 + jnp.exp(-z))

    def feed_forward(k, scale, offset, spans):
        parts = []
        for at, n in spans:
            rows = slice(at, at + n)
            x = st[rows] + att[rows, offset : offset + W]
            if scale is not None:
                x = x + ex[rows] * scale.reshape(1, 1, L)
            parts.append(x)
        x = jnp.concatenate(parts, axis=0)
        u = layer_norm(x).astype(BF16).reshape(8 * W, L)
        h = gelu(dot(u, m1[k])).astype(BF16)
        y = x + dot(h, m2[k]).reshape(8, W, L)
        done = 0
        for at, n in spans:
            part = y[done : done + n]
            done += n
            if k < 3:
                st[at : at + n] = part
                normalize(k + 1, part, pl.ds(at, n))
            else:
                out[at : at + n] = part[:, :, :C].astype(out.dtype)

    def block_end(k, scale, offset, g):
        feed_forward(k, scale, offset, ((0, 4), (12, 4)))
        rows = send_rows(g) if k < 3 else None
        feed_forward(k, scale, offset, ((4, 8),))
        sides = send_sides(g) if k < 3 else None
        return rows, sides

    st[...] = jnp.zeros_like(st)
    st[:, :, :C] = tok[...].astype(F32)

    for i in range(2):
        normalize(0, st[8 * i : 8 * i + 8], pl.ds(8 * i, 8))
    pl.semaphore_wait(barrier, len(peers))
    rows, sides = send_rows(0), send_sides(0)
    finish(loads)
    prepare_attention(0)
    prepare_conv(0)
    prepare_mlp(0)
    prepare_attention(1)
    project_plain(0, (qs, ks, vs))
    lax.fori_loop(0, 1, plain_window(0), 0)
    finish(rows)
    finish(sides)
    receive_rows(0, ue, None)
    receive_sides(0, ue, None)
    conv_in(0)
    ara[0, 0] = conv_out(0)
    copies = stage_a(0)
    start(copies)
    lax.fori_loop(1, 4, plain_window(0), 0)
    copies = between(0, copies)
    prepare_conv(1)
    prepare_mlp(1)
    prepare_attention(2)
    prepare_conv(2)
    rows, sides = block_end(0, gate(0, copies), 0, 1)

    more = send_rows(2)
    project_inner(1, ua, ((0, qe, 8), (1, ke, 0), (2, ve, 0)))
    shifted_near(1, 6, 3, 1, 1)
    finish(sides)
    receive_sides(1, ue, ua)
    project_sides(1, ua, ((0, qe, 8), (1, ke, 0), (2, ve, 0)))
    finish(rows)
    receive_rows(1, ue, ua)
    conv_in(1)
    ara[1, 0] = conv_out(1)
    copies = stage_a(1)
    start(copies)
    shifted_near(1, 4, 2, 0, 4)
    finish(more)
    receive_rows(2, None, ua)
    project_rows(1, ua, 8)
    copies = between(1, copies)
    lax.fori_loop(0, 10, shifted_far(1), 0)
    rows, sides = block_end(1, gate(1, copies), 8, 3)

    project_plain(2, (qs, ks, vs))
    lax.fori_loop(0, 2, plain_window(2), 0)
    finish(sides)
    finish(rows)
    receive_sides(3, ue, None)
    receive_rows(3, ue, None)
    conv_in(2)
    ara[2, 0] = conv_out(2)
    copies = stage_a(2)
    start(copies)
    lax.fori_loop(2, 4, plain_window(2), 0)
    copies = between(2, copies)
    prepare_mlp(2)
    prepare_attention(3)
    prepare_mlp(3)
    rows, sides = block_end(2, gate(2, copies), 0, 4)

    project_plain(3, (qs,))
    project_inner(3, ue, ((1, ke, 0), (2, ve, 0)))
    cross_near(3, 1, 1)
    finish(sides)
    receive_sides(4, ue, None)
    project_sides(3, ue, ((1, ke, 0), (2, ve, 0)))
    cross_near(3, 0, 3)
    finish(rows)
    receive_rows(4, ue, None)
    project_rows(3, ue, 4)
    lax.fori_loop(0, 4, cross_far(3), 0)
    block_end(3, None, 0, None)


def local(tok, qkv, proj, squeeze, expand, down, up_, mlp_in, mlp_out, oqkv, oproj):
    args = (
        tok, qkv, proj, squeeze.transpose(0, 1, 3, 2), expand, down.transpose(0, 2, 1), up_,
        mlp_in.transpose(1, 0, 2), mlp_out.transpose(2, 0, 1), oqkv, oproj,
    )
    vmem = pl.BlockSpec(memory_space=pltpu.VMEM)
    hbm = pl.BlockSpec(memory_space=pltpu.HBM)
    scratch = [pltpu.VMEM(a.shape, a.dtype) for a in args[1:]]
    scratch += [
        pltpu.VMEM((4, 3, L, L), BF16),
        pltpu.VMEM((4, L, L), BF16),
        pltpu.VMEM((3, 3, L, L), BF16),
        pltpu.VMEM((3, 3, L, L), BF16),
        pltpu.VMEM((3, 8, L), F32),
        pltpu.VMEM((3, 8, L), F32),
        pltpu.VMEM((4, L, HL), BF16),
        pltpu.VMEM((4, HL, L), BF16),
        pltpu.VMEM((L, HL), BF16),
        pltpu.VMEM((10, 128, L), F32),
        pltpu.VMEM((10, 128, L), F32),
        pltpu.VMEM((10, 128, L), F32),
        pltpu.VMEM((H, W, L), F32),
        pltpu.VMEM((H, W, L), BF16),
        pltpu.VMEM((32, E, L), BF16),
        pltpu.VMEM((32, E, L), BF16),
        pltpu.VMEM((H, W, L), BF16),
        pltpu.VMEM((H, W, L), BF16),
        pltpu.VMEM((H, W, L), BF16),
        pltpu.VMEM((H, E, L), BF16),
        pltpu.VMEM((32, E, L), BF16),
        pltpu.VMEM((32, E, L), BF16),
        pltpu.VMEM((H, E, L), F32),
        pltpu.VMEM((H, W, L), F32),
        pltpu.VMEM((18, E, 128), F32),
        pltpu.VMEM((3, ROWS, 1, L), F32),
        pltpu.VMEM((3, COLS, 1, L), F32),
    ]
    for _, n, _ in GROUPS:
        for shape in ((2, packed(n), W, 128), (2, packed(8), 16, 128), (4, packed(n // 2), 16, 128)):
            scratch += [pltpu.VMEM(shape, BF16)] * 2
    dma = pltpu.SemaphoreType.DMA
    scratch += [dma((10,)), dma((len(GROUPS), 8)), dma((len(GROUPS), 8))]
    scratch += [dma((3, ROWS)), dma((3, ROWS)), dma((3, COLS)), dma((3, COLS))]
    return pl.pallas_call(
        kernel,
        out_shape=jax.ShapeDtypeStruct((H, W, C), BF16),
        in_specs=[vmem] + [hbm] * 10,
        out_specs=vmem,
        scratch_shapes=scratch,
        compiler_params=pltpu.CompilerParams(
            collective_id=0, has_side_effects=True, vmem_limit_bytes=60 * 1024 * 1024
        ),
        name="blocks",
    )(*args)


def solution(mesh):
    placed = (P("row", "col", None),) + (P(),) * 10
    return jax.shard_map(
        local, mesh=mesh, in_specs=placed, out_specs=P("row", "col", None), check_vma=False
    )
```

```python
import jax
import jax.numpy as jnp
from jax import lax
from jax.experimental import pallas as pl
from jax.experimental.pallas import tpu as pltpu
from jax.sharding import PartitionSpec as P

C = 180
HEADS = 6
HD = C // HEADS
WIN = 16
L = 256
HID = 360
HL = 384
ROWS = 8
COLS = 16
H = 16
W = 64
E = 80
EPSILON = 1e-05
BIG = -1e30
QSCALE = HD ** (-0.5) * 1.4426950408889634
F32 = jnp.float32
BF16 = jnp.bfloat16
MESH = pl.DeviceIdType.MESH
GROUPS = ((0, 2, True), (0, 2, True), (2, 6, False), (0, 2, True), (0, 4, True))


def dot(a, b):
    return jnp.dot(a, b, preferred_element_type=F32)


def dot_t(a, b):
    return lax.dot_general(a, b, (((1,), (1,)), ((), ())), preferred_element_type=F32)


def gelu(v):
    return v * (1.0 + lax.erf(v * 0.7071067811865476)) * 0.5


def iota(shape, dim):
    return lax.broadcasted_iota(jnp.int32, shape, dim)


def layer_norm(x):
    nd = x.ndim
    inside = iota((1,) * (nd - 1) + (L,), nd - 1) < C
    mean = jnp.sum(x, axis=-1, keepdims=True) * (1.0 / C)
    centered = jnp.where(inside, x - mean, 0.0)
    spread = jnp.sum(centered * centered, axis=-1, keepdims=True) * (1.0 / C)
    return centered * lax.rsqrt(spread + EPSILON)


def attend_part(q, k, v, group):
    tq = q.shape[0]
    lane = iota((1, L), 1)
    num = top = den = None
    for first in range(0, HEADS, group):
        stacked = []
        for h in range(first, first + group):
            mask = ((lane >= h * HD) & (lane < h * HD + HD)) | (lane >= C)
            stacked.append(q * mask.astype(F32).astype(BF16))
        s = dot_t(jnp.concatenate(stacked, axis=0), k)
        m = jnp.max(s, axis=-1, keepdims=True)
        p = jnp.exp2(s - m)
        d = jnp.sum(p, axis=-1, keepdims=True)
        r = dot(p.astype(BF16), v)
        for i in range(group):
            span = slice(i * tq, (i + 1) * tq)
            here = lane >= (first + i) * HD
            wide = [r[span], jnp.broadcast_to(m[span], (tq, L)), jnp.broadcast_to(d[span], (tq, L))]
            if num is None:
                num, top, den = wide
            else:
                num, top, den = (jnp.where(here, x, y) for x, y in zip(wide, (num, top, den)))
    return num, top, den


def attend(q, k, v, group):
    num, _, den = attend_part(q, k, v, group)
    return (num / den).astype(BF16)


def merge_parts(a, b):
    (n0, m0, d0), (n1, m1, d1) = a, b
    m = jnp.maximum(m0, m1)
    c0, c1 = jnp.exp2(m0 - m), jnp.exp2(m1 - m)
    return ((n0 * c0 + n1 * c1) / (d0 * c0 + d1 * c1)).astype(BF16)


def packed(n):
    return n + (n + 1) // 2


def pack(x, ref):
    n = x.shape[0]
    half = (n + 1) // 2
    ref[0:n] = x[:, :, :128].astype(BF16)
    low = x[:half, :, 128:]
    if n > half:
        high = pltpu.roll(x[half:, :, 128:], 64, 2)
        if n < 2 * half:
            high = jnp.concatenate([high, jnp.zeros_like(low[:1])], axis=0)
        low = low + high
    ref[n : n + half] = low.astype(BF16)


def unpack(ref, n):
    half = (n + 1) // 2
    upper = iota((1, 1, 128), 2) < C - 128
    both = ref[n : n + half].astype(F32)
    b = jnp.where(upper, both, 0.0)
    if n > half:
        high = jnp.where(upper, pltpu.roll(both, 64, 2), 0.0)
        b = jnp.concatenate([b, high[: n - half]], axis=0)
    return jnp.concatenate([ref[0:n].astype(F32), b], axis=2)


def fold(x):
    m = x.shape[0] // 2
    return jnp.concatenate([x[:m], x[m:]], axis=1)


def unfold(x):
    return jnp.concatenate([x[:, :8], x[:, 8:]], axis=0)


def kernel(*refs):
    (
        tok, qkv_h, proj_h, sq_h, ex_h, gd_h, gu_h, m1_h, m2_h, oqkv_h, oproj_h, out,
        rqkv, rproj, rsq, rex, rgd, rgu, rm1, rm2, roqkv, roproj,
        wqkv, wp, w1, w2, gd, gu, m1, m2, tmp, pn, pm, pd,
        st, un, ue, ua, qs, ks, vs, qe, ke, ve, oe, att, ex, h32, arf,
    ) = refs[:49]
    bufs = refs[49 : 49 + 6 * len(GROUPS)]
    wsem, hs, hr, asend, arecv, ready = refs[49 + 6 * len(GROUPS) :]
    row_s, row_r, col_s, col_r, cor_s, cor_r = (bufs[i :: 6] for i in range(6))
    row = lax.axis_index("row")
    col = lax.axis_index("col")
    up, down = lax.rem(row + ROWS - 1, ROWS), lax.rem(row + 1, ROWS)
    left, right = lax.rem(col + COLS - 1, COLS), lax.rem(col + 1, COLS)

    barrier = pltpu.get_barrier_semaphore()
    others = ROWS * COLS - 1

    def peer(dr, dc):
        return lax.rem(row + dr, ROWS), lax.rem(col + dc, COLS)

    def for_others(act):
        for dr in (4, 3, 5, 2, 6, 1, 7, 0):

            def step(i, carry, dr=dr):
                act(dr, lax.rem(i + COLS // 2, COLS))
                return carry

            if dr:
                lax.fori_loop(0, COLS, step, 0, unroll=4)
            else:
                lax.fori_loop(0, COLS // 2, step, 0)
                lax.fori_loop(COLS // 2 + 1, COLS, step, 0)

    peers = [peer(d, 0) for d in range(1, ROWS)] + [peer(0, d) for d in range(1, COLS)]
    peers += [(up, left), (up, right), (down, left), (down, right)]
    for p in peers:
        pl.semaphore_signal(barrier, inc=1, device_id=p, device_id_type=MESH)

    loads = [
        pltpu.make_async_copy(s, d, wsem.at[i])
        for i, (s, d) in enumerate(
            [
                (qkv_h, rqkv), (proj_h, rproj), (sq_h, rsq), (ex_h, rex), (gd_h, rgd),
                (gu_h, rgu), (m1_h, rm1), (m2_h, rm2), (oqkv_h, roqkv), (oproj_h, roproj),
            ]
        )
    ]
    for c in loads:
        c.start()

    def remote(src, dst, send, recv, peer):
        return pltpu.make_async_remote_copy(
            src_ref=src, dst_ref=dst, send_sem=send, recv_sem=recv, device_id=peer, device_id_type=MESH
        )

    def start(copies):
        for c in copies:
            c.start()

    def finish(copies):
        for c in copies:
            c.wait()


    def prepare_attention(k):
        w = rqkv.at[k] if k < 3 else roqkv
        zero = jnp.zeros((L, L), BF16)
        for i in range(3):
            wqkv[k, i] = zero
        whole = w[...]
        wqkv[k, 0, 0:C, 0:C] = w[:, 0:C]
        for i in range(1, 3):
            pick = (iota((3 * C, L), 0) == iota((3 * C, L), 1) + i * C) & (iota((3 * C, L), 1) < C)
            wqkv[k, i, 0:C] = dot(whole, jnp.where(pick, 1.0, 0.0).astype(BF16)).astype(BF16)
        wp[k] = zero
        wp[k, 0:C, 0:C] = rproj[k] if k < 3 else roproj[...]

    def prepare_conv(k):
        zero = jnp.zeros((L, L), BF16)
        for a in range(3):
            tmp[:, 0:L] = zero
            for b in range(3):
                tmp[64 * b : 64 * b + 60, 0:C] = rsq[k, 3 * a + b]
            w1[k, a] = tmp[:, 0:L].astype(F32).T.astype(BF16)
        for b in range(3):
            w2[k, b] = zero
            for a in range(3):
                w2[k, b, 64 * a : 64 * a + 60, 0:C] = rex[k, 3 * a + b]
        for dst, raw in ((gd, rgd), (gu, rgu)):
            dst[k] = jnp.zeros((8, L), F32)
            dst[k, 0:6, 0:C] = raw[k].astype(F32)

    def prepare_mlp(k):
        m1[k] = jnp.zeros((L, HL), BF16)
        m1[k, 0:C, 0:HID] = rm1[:, k, :]
        tmp[...] = jnp.zeros((L, HL), BF16)
        tmp[0:C, 0:HID] = rm2[:, k, :]
        m2[k] = tmp[...].astype(F32).T.astype(BF16)


    def copies_of(g, which):
        plan = [
            (row_s[g].at[0], row_r[g].at[0], (up, col)),
            (row_s[g].at[1], row_r[g].at[1], (down, col)),
            (col_s[g].at[0], col_r[g].at[0], (row, left)),
            (col_s[g].at[1], col_r[g].at[1], (row, right)),
            (cor_s[g].at[0], cor_r[g].at[0], (up, left)),
            (cor_s[g].at[1], cor_r[g].at[1], (up, right)),
            (cor_s[g].at[2], cor_r[g].at[2], (down, left)),
            (cor_s[g].at[3], cor_r[g].at[3], (down, right)),
        ]
        return [
            remote(s, d, hs.at[g, i], hr.at[g, i], p)
            for i, (s, d, p) in enumerate(plan)
            if i in which
        ]

    def send_rows(g):
        d0, n, _ = GROUPS[g]
        top = un[d0 : d0 + n].astype(F32)
        low = un[H - d0 - n : H - d0].astype(F32)
        pack(top, row_s[g].at[0])
        pack(low, row_s[g].at[1])
        pack(fold(top[:, 0:8]), cor_s[g].at[0])
        pack(fold(top[:, W - 8 : W]), cor_s[g].at[1])
        pack(fold(low[:, 0:8]), cor_s[g].at[2])
        pack(fold(low[:, W - 8 : W]), cor_s[g].at[3])
        low_half, top_half = copies_of(g, (1, 6, 7)), copies_of(g, (0, 4, 5))
        start(low_half)
        start(top_half)
        return low_half, top_half

    def send_sides(g):
        pack(fold(un[:, 0:16].astype(F32)[:, 0:8]), col_s[g].at[0])
        pack(fold(un[:, W - 16 : W].astype(F32)[:, 8:16]), col_s[g].at[1])
        sides = copies_of(g, (2, 3))
        start(sides)
        return sides

    yes_up = jnp.where(row > 0, 1.0, 0.0)
    yes_down = jnp.where(row < ROWS - 1, 1.0, 0.0)
    yes_left = jnp.where(col > 0, 1.0, 0.0)
    yes_right = jnp.where(col < COLS - 1, 1.0, 0.0)

    def receive_rows(g, masked, whole, sides=(1, 0)):
        d0, n, _ = GROUPS[g]
        m = n // 2
        for which, lc, rc, at, keep in ((1, 3, 2, 8 - d0 - n, yes_up), (0, 1, 0, 24 + d0, yes_down)):
            if which not in sides:
                continue
            mid = unpack(row_r[g].at[which], n)
            lcorner = unfold(unpack(cor_r[g].at[lc], m))
            rcorner = unfold(unpack(cor_r[g].at[rc], m))
            if whole is not None:
                whole[at : at + n] = jnp.concatenate([lcorner, mid, rcorner], axis=1).astype(BF16)
            if masked is not None:
                masked[at : at + n] = jnp.concatenate(
                    [lcorner * (keep * yes_left), mid * keep, rcorner * (keep * yes_right)], axis=1
                ).astype(BF16)

    def receive_sides(g, masked, whole):
        lside = unfold(unpack(col_r[g].at[1], 8))
        rside = unfold(unpack(col_r[g].at[0], 8))
        first = un[:, 0:16].astype(F32)[:, 0:8]
        last = un[:, W - 16 : W].astype(F32)[:, 8:16]
        if whole is not None:
            whole[8:24, 0:16] = jnp.concatenate([lside, first], axis=1).astype(BF16)
            whole[8:24, 64:80] = jnp.concatenate([last, rside], axis=1).astype(BF16)
        if masked is not None:
            masked[8:24, 0:16] = jnp.concatenate([lside * yes_left, first], axis=1).astype(BF16)
            masked[8:24, 64:80] = jnp.concatenate([last, rside * yes_right], axis=1).astype(BF16)

    def normalize(k, y, rows):
        u = layer_norm(y)
        un[rows] = u.astype(BF16)
        inner = u[:, 8:56].astype(BF16)
        at = pl.ds(rows.start + 8, rows.size)
        ue[at, 16:64] = inner
        if k == 1:
            ua[at, 16:64] = inner

    def project(k, which, x):
        r, c, _ = x.shape
        y = dot(x.reshape(r * c, L), wqkv[k, which])
        if which == 0:
            y = y * QSCALE
        return y.astype(BF16).reshape(r, c, L)

    def project_plain(k, dsts):
        def step(i, carry):
            rows = pl.ds(i * 8, 8)
            x = un[rows]
            for which, dst in enumerate(dsts):
                dst[rows] = project(k, which, x)
            return carry

        lax.fori_loop(0, 2, step, 0)

    def project_inner(k, src, dsts):
        def step(i, carry):
            x = src[pl.ds(8 + 8 * i, 8), 16:64]
            for which, dst, base in dsts:
                dst[pl.ds(8 - base + 8 * i, 8), 16:64] = project(k, which, x)
            return carry

        lax.fori_loop(0, 2, step, 0)

    def project_sides(k, src, dsts):
        x = jnp.concatenate([src[8:24, 0:16], src[8:24, 64:80]], axis=1)
        for which, dst, base in dsts:
            y = project(k, which, x)
            dst[8 - base : 24 - base, 0:16] = y[:, 0:16]
            dst[8 - base : 24 - base, 64:80] = y[:, 16:32]

    def project_rows(k, src, n, sides=(1, 0)):
        for at in [(24, 8 - n)[side] for side in sides]:
            x = src[at : at + n]
            for which, dst in ((1, ke), (2, ve)):
                dst[at : at + n] = project(k, which, x)


    def plain_window(k):
        def step(w, carry):
            cols = pl.ds(pl.multiple_of(w * WIN, WIN), WIN)
            q = qs[:, cols].reshape(WIN * WIN, L)
            kk = ks[:, cols].reshape(WIN * WIN, L)
            vv = vs[:, cols].reshape(WIN * WIN, L)
            o = attend(q, kk, vv, HEADS)
            att[:, cols] = dot(o, wp[k]).reshape(WIN, WIN, L)
            return carry

        return step

    def shifted_windows(k, ry):
        lane = iota((1, 1, L), 2)
        qcol = iota((8, WIN, 1), 1) >= 8
        qpat = jnp.where(lane == C, 1.0, 0.0) + jnp.where(
            ((lane == C + 1) & ~qcol) | ((lane == C + 2) & qcol), 1.0, 0.0
        )
        krow = iota((WIN, WIN, 1), 0) >= 8
        kcol = iota((WIN, WIN, 1), 1) >= 8
        differs = krow if ry == 1 else ~krow
        brow = jnp.where(row == (ROWS - 1 if ry == 1 else 0), BIG, 0.0)
        rbias = jnp.where((lane == C) & differs, brow, 0.0)
        for w in range(5):
            cols = slice(w * WIN, (w + 1) * WIN)
            bias = rbias
            if w in (0, 4):
                bcol = jnp.where(col == (COLS - 1 if w == 4 else 0), BIG, 0.0)
                bias = bias + jnp.where(((lane == C + 1) & kcol) | ((lane == C + 2) & ~kcol), bcol, 0.0)
            q = (qe[8 * ry : 8 * ry + 8, cols].astype(F32) + qpat).astype(BF16)
            kk = (ke[WIN * ry : WIN * ry + WIN, cols].astype(F32) + bias).astype(BF16)
            vv = ve[WIN * ry : WIN * ry + WIN, cols]
            o = attend(q.reshape(8 * WIN, L), kk.reshape(WIN * WIN, L), vv.reshape(WIN * WIN, L), HEADS)
            oe[8 * ry : 8 * ry + 8, cols] = o.reshape(8, WIN, L)
        o = oe[8 * ry : 8 * ry + 8].reshape(8 * E, L)
        att[8 * ry : 8 * ry + 8] = dot(o, wp[k]).reshape(8, E, L)

    def cross_part(w, rows):
        lane = iota((1, 1, L), 2)
        qpat = jnp.where(lane == C, 1.0, 0.0)
        kcol = iota((1, 32, 1), 1)
        bias = jnp.where((lane == C) & ((kcol < 4) | (kcol >= 28)), BIG, 0.0)
        cols = slice(w * WIN, (w + 1) * WIN)
        wide = slice(w * WIN, w * WIN + 32)
        q = (qs[:, cols].astype(F32) + qpat).astype(BF16).reshape(WIN * WIN, L)
        kk = jnp.concatenate([ke[r, wide] for r in rows], axis=0)
        vv = jnp.concatenate([ve[r, wide] for r in rows], axis=0)
        n = kk.shape[0] * 32
        kk = (kk.astype(F32) + bias).astype(BF16).reshape(n, L)
        return attend_part(q, kk, vv.reshape(n, L), 2)

    def cross_near(windows):
        for w in windows:
            part = cross_part(w, (slice(8, 24),))
            for ref, value in zip((pn, pm, pd), part):
                ref[w] = value

    def cross_far(k):
        for w in range(4):
            far = cross_part(w, (slice(4, 8), slice(24, 28)))
            o = merge_parts(tuple(ref[w] for ref in (pn, pm, pd)), far)
            oe[:, w * WIN : (w + 1) * WIN] = o.reshape(WIN, WIN, L)
        o = oe[:, 0:W].reshape(H * W, L)
        att[:, 0:W] = dot(o, wp[k]).reshape(H, W, L)


    def conv_in(k):
        chunk = 9
        hrow = iota((chunk, E, 1), 0)
        hcol = iota((chunk, E, 1), 1)
        lane = iota((1, 1, 128), 2)
        low = jnp.where(col == 0, 8, 0)
        high = jnp.where(col == COLS - 1, 72, E)
        rlow = jnp.where(row == 0, 1, 0)
        rhigh = jnp.where(row == ROWS - 1, 17, 18)

        def step(i, carry):
            acc = None
            for a in range(3):
                x = ue[pl.ds(6 + a + i * chunk, chunk)].reshape(chunk * E, L)
                y = dot(x, w1[k, a])
                acc = y if acc is None else acc + y
            r = acc.reshape(chunk, E, L)
            first, second = r[:, :, :128], r[:, :, 128:]
            s = pltpu.roll(first, 1, 1) + pltpu.roll(first, 64, 2) + pltpu.roll(second, E - 1, 1)
            g = gelu(s)
            at = hrow + i * chunk
            ok = (at >= rlow) & (at < rhigh) & (hcol >= low) & (hcol < high) & (lane < 60)
            h32[pl.ds(i * chunk, chunk)] = jnp.where(ok, g, 0.0).astype(BF16).astype(F32)
            return carry

        for i in range(18 // chunk):
            step(i, 0)

    def conv_out(k):
        chunk = 8

        def step(i, carry):
            lead = h32[pl.ds(i * chunk, chunk)]
            mid = h32[pl.ds(i * chunk + 1, chunk)]
            tail = h32[pl.ds(i * chunk + 2, chunk)]
            x = jnp.concatenate([lead + pltpu.roll(mid, 64, 2), tail], axis=2)
            x = x.astype(BF16).reshape(chunk * E, L)
            r0 = dot(x, w2[k, 0]).reshape(chunk, E, L)
            r1 = dot(x, w2[k, 1]).reshape(chunk, E, L)
            r2 = dot(x, w2[k, 2]).reshape(chunk, E, L)
            y = (pltpu.roll(r0, 1, 1) + r1 + pltpu.roll(r2, E - 1, 1))[:, 8:72]
            ex[pl.ds(i * chunk, chunk)] = y
            return carry

        lax.fori_loop(0, H // chunk, step, 0)


    is_top, is_low = 1.0 - yes_up, 1.0 - yes_down
    is_left, is_right = 1.0 - yes_left, 1.0 - yes_right

    def expanded_sum(k):
        def over(x):
            return jnp.sum(jnp.sum(x, axis=0), axis=0, keepdims=True)

        every = over(h32[1:17, 8:72])
        top, low = over(h32[1:2, 8:72]) * is_top, over(h32[16:17, 8:72]) * is_low
        lead, tail = h32[1:17, 8:16][:, 0:1], h32[1:17, 64:72][:, 7:8]
        left_, right_ = over(lead) * is_left, over(tail) * is_right
        rows_out = (low, None, top)
        cols_out = (right_, None, left_)
        corner = {
            (0, 0): tail[15] * (is_low * is_right),
            (0, 2): lead[15] * (is_low * is_left),
            (2, 0): tail[0] * (is_top * is_right),
            (2, 2): lead[0] * (is_top * is_left),
        }
        total = None
        for b in range(3):
            s = []
            for a in range(3):
                v = every
                if rows_out[a] is not None:
                    v = v - rows_out[a]
                if cols_out[b] is not None:
                    v = v - cols_out[b]
                if (a, b) in corner:
                    v = v + corner[a, b]
                s.append(v)
            v = jnp.concatenate([s[0] + pltpu.roll(jnp.broadcast_to(s[1], (8, 128)), 64, 1)[0:1], s[2]], axis=1)
            first = v.astype(BF16).astype(F32)
            second = (v - first).astype(BF16).astype(F32)
            third = v - first - second
            x = jnp.concatenate([first, second, third, jnp.zeros((5, L), F32)], axis=0).astype(BF16)
            y = jnp.sum(dot(x, w2[k, b]), axis=0, keepdims=True)
            total = y if total is None else total + y
        return total

    def spread(k, part):
        arf[k, 0] = part

        def one(dr, dc):
            slot = dr * COLS + dc
            remote(arf.at[k, 0], arf.at[k, slot], asend.at[k], arecv.at[k], peer(dr, dc)).start()

        for_others(one)

    def gate(k):
        rest = arf.at[k, pl.ds(1, others)]
        remote(rest, rest, asend.at[k], arecv.at[k], (row, col)).wait()
        s = jnp.sum(arf[k], axis=0)
        pooled = s * (1.0 / (ROWS * COLS * H * W))
        squeezed = jnp.sum(gd[k] * pooled, axis=-1, keepdims=True)
        squeezed = jnp.maximum(squeezed, 0.0)
        z = jnp.sum(gu[k] * squeezed, axis=0, keepdims=True)
        return 1.0 / (1.0 + jnp.exp(-z))

    def feed_forward(k, scale, offset, spans):
        parts = []
        for at, n in spans:
            rows = slice(at, at + n)
            x = st[rows] + att[rows, offset : offset + W]
            if scale is not None:
                x = x + ex[rows] * scale.reshape(1, 1, L)
            parts.append(x)
        x = jnp.concatenate(parts, axis=0)
        u = layer_norm(x).astype(BF16).reshape(8 * W, L)
        h = gelu(dot(u, m1[k])).astype(BF16)
        y = x + dot(h, m2[k]).reshape(8, W, L)
        done = 0
        for at, n in spans:
            part = y[done : done + n]
            done += n
            if k < 3:
                st[at : at + n] = part
                normalize(k + 1, part, pl.ds(at, n))
            else:
                out[at : at + n] = part[:, :, :C].astype(out.dtype)

    def block_end(k, scale, offset, g):
        feed_forward(k, scale, offset, ((0, 4), (12, 4)))
        rows = send_rows(g) if k < 3 else None
        feed_forward(k, scale, offset, ((4, 8),))
        sides = send_sides(g) if k < 3 else None
        return rows, sides

    st[...] = jnp.zeros_like(st)
    st[:, :, :C] = tok[...].astype(F32)

    for i in range(2):
        normalize(0, st[8 * i : 8 * i + 8], pl.ds(8 * i, 8))
    pl.semaphore_wait(barrier, len(peers))
    rows, sides = send_rows(0), send_sides(0)
    for d in range(1, COLS):
        pl.semaphore_signal(ready, inc=1, device_id=peer(0, d), device_id_type=MESH)
    finish(loads)
    prepare_attention(0)
    prepare_conv(0)
    project_plain(0, (qs, ks, vs))
    prepare_mlp(0)
    prepare_attention(1)
    prepare_conv(1)
    finish(sides + rows[0] + rows[1])
    receive_sides(0, ue, None)
    receive_rows(0, ue, None)
    conv_in(0)
    part = expanded_sum(0)
    pl.semaphore_wait(ready, COLS - 1)
    spread(0, part)
    conv_out(0)
    lax.fori_loop(0, 4, plain_window(0), 0)
    prepare_mlp(1)
    prepare_attention(2)
    prepare_conv(2)
    prepare_mlp(2)
    rows, sides = block_end(0, gate(0), 0, 1)

    more = send_rows(2)
    project_inner(1, ua, ((0, qe, 8), (1, ke, 0), (2, ve, 0)))
    finish(sides)
    receive_sides(1, ue, ua)
    project_sides(1, ua, ((0, qe, 8), (1, ke, 0), (2, ve, 0)))
    finish(rows[0] + rows[1])
    receive_rows(1, ue, ua)
    conv_in(1)
    spread(1, expanded_sum(1))
    conv_out(1)
    finish(more[0])
    receive_rows(2, None, ua, (1,))
    project_rows(1, ua, 8, (1,))
    shifted_windows(1, 0)
    finish(more[1])
    receive_rows(2, None, ua, (0,))
    project_rows(1, ua, 8, (0,))
    shifted_windows(1, 1)
    rows, sides = block_end(1, gate(1), 8, 3)

    project_plain(2, (qs, ks, vs))
    prepare_attention(3)
    prepare_mlp(3)
    finish(sides + rows[0] + rows[1])
    receive_sides(3, ue, None)
    receive_rows(3, ue, None)
    conv_in(2)
    spread(2, expanded_sum(2))
    conv_out(2)
    lax.fori_loop(0, 4, plain_window(2), 0)
    rows, sides = block_end(2, gate(2), 0, 4)

    project_plain(3, (qs,))
    project_inner(3, ue, ((1, ke, 0), (2, ve, 0)))
    cross_near((1, 2))
    finish(sides)
    receive_sides(4, ue, None)
    project_sides(3, ue, ((1, ke, 0), (2, ve, 0)))
    cross_near((0, 3))
    finish(rows[0] + rows[1])
    receive_rows(4, ue, None)
    project_rows(3, ue, 4)
    cross_far(3)
    block_end(3, None, 0, None)


def local(tok, qkv, proj, squeeze, expand, down, up_, mlp_in, mlp_out, oqkv, oproj):
    args = (
        tok, qkv, proj, squeeze.transpose(0, 1, 3, 2), expand, down.transpose(0, 2, 1), up_,
        mlp_in.transpose(1, 0, 2), mlp_out.transpose(2, 0, 1), oqkv, oproj,
    )
    vmem = pl.BlockSpec(memory_space=pltpu.VMEM)
    hbm = pl.BlockSpec(memory_space=pltpu.HBM)
    scratch = [pltpu.VMEM(a.shape, a.dtype) for a in args[1:]]
    scratch += [
        pltpu.VMEM((4, 3, L, L), BF16),
        pltpu.VMEM((4, L, L), BF16),
        pltpu.VMEM((3, 3, L, L), BF16),
        pltpu.VMEM((3, 3, L, L), BF16),
        pltpu.VMEM((3, 8, L), F32),
        pltpu.VMEM((3, 8, L), F32),
        pltpu.VMEM((4, L, HL), BF16),
        pltpu.VMEM((4, HL, L), BF16),
        pltpu.VMEM((L, HL), BF16),
        pltpu.VMEM((4, WIN * WIN, L), F32),
        pltpu.VMEM((4, WIN * WIN, L), F32),
        pltpu.VMEM((4, WIN * WIN, L), F32),
        pltpu.VMEM((H, W, L), F32),
        pltpu.VMEM((H, W, L), BF16),
        pltpu.VMEM((32, E, L), BF16),
        pltpu.VMEM((32, E, L), BF16),
        pltpu.VMEM((H, W, L), BF16),
        pltpu.VMEM((H, W, L), BF16),
        pltpu.VMEM((H, W, L), BF16),
        pltpu.VMEM((H, E, L), BF16),
        pltpu.VMEM((32, E, L), BF16),
        pltpu.VMEM((32, E, L), BF16),
        pltpu.VMEM((H, E, L), BF16),
        pltpu.VMEM((H, E, L), F32),
        pltpu.VMEM((H, W, L), F32),
        pltpu.VMEM((18, E, 128), F32),
        pltpu.VMEM((3, ROWS * COLS, 1, L), F32),
    ]
    for _, n, _ in GROUPS:
        for shape in ((2, packed(n), W, 128), (2, packed(8), 16, 128), (4, packed(n // 2), 16, 128)):
            scratch += [pltpu.VMEM(shape, BF16)] * 2
    dma = pltpu.SemaphoreType.DMA
    scratch += [dma((10,)), dma((len(GROUPS), 8)), dma((len(GROUPS), 8))]
    scratch += [dma((3,)), dma((3,)), pltpu.SemaphoreType.REGULAR]
    return pl.pallas_call(
        kernel,
        out_shape=jax.ShapeDtypeStruct((H, W, C), F32),
        in_specs=[vmem] + [hbm] * 10,
        out_specs=vmem,
        scratch_shapes=scratch,
        compiler_params=pltpu.CompilerParams(
            collective_id=0, has_side_effects=True, vmem_limit_bytes=60 * 1024 * 1024
        ),
        name="blocks",
    )(*args).astype(BF16)


def solution(mesh):
    placed = (P("row", "col", None),) + (P(),) * 10
    return jax.shard_map(
        local, mesh=mesh, in_specs=placed, out_specs=P("row", "col", None), check_vma=False
    )
```

```python
import jax
import jax.numpy as jnp
from jax import lax
from jax.experimental import pallas as pl
from jax.experimental.pallas import tpu as pltpu
from jax.sharding import PartitionSpec as P

C = 180
HEADS = 6
HD = C // HEADS
WIN = 16
L = 256
HID = 360
HL = 384
ROWS = 8
COLS = 16
H = 16
W = 64
E = 80
EPSILON = 1e-05
BIG = -1e30
QSCALE = HD ** (-0.5) * 1.4426950408889634
F32 = jnp.float32
BF16 = jnp.bfloat16
MESH = pl.DeviceIdType.MESH
GROUPS = ((0, 2, True), (0, 2, True), (2, 6, False), (0, 2, True), (0, 4, True))


def dot(a, b):
    return jnp.dot(a, b, preferred_element_type=F32)


def dot_t(a, b):
    return lax.dot_general(a, b, (((1,), (1,)), ((), ())), preferred_element_type=F32)


def gelu(v):
    return v * (1.0 + lax.erf(v * 0.7071067811865476)) * 0.5


def iota(shape, dim):
    return lax.broadcasted_iota(jnp.int32, shape, dim)


def layer_norm(x):
    nd = x.ndim
    inside = iota((1,) * (nd - 1) + (L,), nd - 1) < C
    mean = jnp.sum(x, axis=-1, keepdims=True) * (1.0 / C)
    centered = jnp.where(inside, x - mean, 0.0)
    spread = jnp.sum(centered * centered, axis=-1, keepdims=True) * (1.0 / C)
    return centered * lax.rsqrt(spread + EPSILON)


def attend_part(q, k, v, group):
    tq = q.shape[0]
    lane = iota((1, L), 1)
    num = top = den = None
    for first in range(0, HEADS, group):
        stacked = []
        for h in range(first, first + group):
            mask = ((lane >= h * HD) & (lane < h * HD + HD)) | (lane >= C)
            stacked.append(q * mask.astype(F32).astype(BF16))
        s = dot_t(jnp.concatenate(stacked, axis=0), k)
        m = jnp.max(s, axis=-1, keepdims=True)
        p = jnp.exp2(s - m)
        d = jnp.sum(p, axis=-1, keepdims=True)
        r = dot(p.astype(BF16), v)
        for i in range(group):
            span = slice(i * tq, (i + 1) * tq)
            here = lane >= (first + i) * HD
            wide = [r[span], jnp.broadcast_to(m[span], (tq, L)), jnp.broadcast_to(d[span], (tq, L))]
            if num is None:
                num, top, den = wide
            else:
                num, top, den = (jnp.where(here, x, y) for x, y in zip(wide, (num, top, den)))
    return num, top, den


def attend(q, k, v, group):
    num, _, den = attend_part(q, k, v, group)
    return (num / den).astype(BF16)


def merge_parts(a, b):
    (n0, m0, d0), (n1, m1, d1) = a, b
    m = jnp.maximum(m0, m1)
    c0, c1 = jnp.exp2(m0 - m), jnp.exp2(m1 - m)
    return ((n0 * c0 + n1 * c1) / (d0 * c0 + d1 * c1)).astype(BF16)


def packed(n):
    return n + (n + 1) // 2


def pack(x, ref):
    n = x.shape[0]
    half = (n + 1) // 2
    ref[0:n] = x[:, :, :128].astype(BF16)
    low = x[:half, :, 128:]
    if n > half:
        high = pltpu.roll(x[half:, :, 128:], 64, 2)
        if n < 2 * half:
            high = jnp.concatenate([high, jnp.zeros_like(low[:1])], axis=0)
        low = low + high
    ref[n : n + half] = low.astype(BF16)


def unpack(ref, n):
    half = (n + 1) // 2
    upper = iota((1, 1, 128), 2) < C - 128
    both = ref[n : n + half].astype(F32)
    b = jnp.where(upper, both, 0.0)
    if n > half:
        high = jnp.where(upper, pltpu.roll(both, 64, 2), 0.0)
        b = jnp.concatenate([b, high[: n - half]], axis=0)
    return jnp.concatenate([ref[0:n].astype(F32), b], axis=2)


def fold(x):
    m = x.shape[0] // 2
    return jnp.concatenate([x[:m], x[m:]], axis=1)


def unfold(x):
    return jnp.concatenate([x[:, :8], x[:, 8:]], axis=0)


def kernel(*refs):
    (
        tok, qkv_h, proj_h, sq_h, ex_h, gd_h, gu_h, m1_h, m2_h, oqkv_h, oproj_h, out,
        rqkv, rproj, rsq, rex, rgd, rgu, rm1, rm2, roqkv, roproj,
        wqkv, wp, w1, w2, gd, gu, m1, m2, tmp, pn, pm, pd,
        st, uf, un, ue, ua, qs, ks, vs, qe, ke, ve, oe, att, ex, h32, arf,
    ) = refs[:50]
    bufs = refs[50 : 50 + 6 * len(GROUPS)]
    wsem, hs, hr, asend, arecv, ready = refs[50 + 6 * len(GROUPS) :]
    row_s, row_r, col_s, col_r, cor_s, cor_r = (bufs[i :: 6] for i in range(6))
    row = lax.axis_index("row")
    col = lax.axis_index("col")
    up, down = lax.rem(row + ROWS - 1, ROWS), lax.rem(row + 1, ROWS)
    left, right = lax.rem(col + COLS - 1, COLS), lax.rem(col + 1, COLS)

    barrier = pltpu.get_barrier_semaphore()
    others = ROWS * COLS - 1

    def peer(dr, dc):
        return lax.rem(row + dr, ROWS), lax.rem(col + dc, COLS)

    def for_others(act):
        for dr in (4, 3, 5, 2, 6, 1, 7, 0):

            def step(i, carry, dr=dr):
                act(dr, lax.rem(i + COLS // 2, COLS))
                return carry

            if dr:
                lax.fori_loop(0, COLS, step, 0, unroll=4)
            else:
                lax.fori_loop(0, COLS // 2, step, 0)
                lax.fori_loop(COLS // 2 + 1, COLS, step, 0)

    peers = [peer(d, 0) for d in range(1, ROWS)] + [peer(0, d) for d in range(1, COLS)]
    peers += [(up, left), (up, right), (down, left), (down, right)]
    for p in peers:
        pl.semaphore_signal(barrier, inc=1, device_id=p, device_id_type=MESH)

    loads = [
        pltpu.make_async_copy(s, d, wsem.at[i])
        for i, (s, d) in enumerate(
            [
                (qkv_h, rqkv), (proj_h, rproj), (sq_h, rsq), (ex_h, rex), (gd_h, rgd),
                (gu_h, rgu), (m1_h, rm1), (m2_h, rm2), (oqkv_h, roqkv), (oproj_h, roproj),
            ]
        )
    ]
    for c in loads:
        c.start()

    def remote(src, dst, send, recv, peer):
        return pltpu.make_async_remote_copy(
            src_ref=src, dst_ref=dst, send_sem=send, recv_sem=recv, device_id=peer, device_id_type=MESH
        )

    def start(copies):
        for c in copies:
            c.start()

    def finish(copies):
        for c in copies:
            c.wait()


    def prepare_attention(k):
        w = rqkv.at[k] if k < 3 else roqkv
        zero = jnp.zeros((L, L), BF16)
        for i in range(3):
            wqkv[k, i] = zero
        whole = w[...]
        wqkv[k, 0, 0:C, 0:C] = w[:, 0:C]
        for i in range(1, 3):
            pick = (iota((3 * C, L), 0) == iota((3 * C, L), 1) + i * C) & (iota((3 * C, L), 1) < C)
            wqkv[k, i, 0:C] = dot(whole, jnp.where(pick, 1.0, 0.0).astype(BF16)).astype(BF16)
        wp[k] = zero
        wp[k, 0:C, 0:C] = rproj[k] if k < 3 else roproj[...]

    def prepare_conv(k):
        zero = jnp.zeros((L, L), BF16)
        for a in range(3):
            tmp[:, 0:L] = zero
            for b in range(3):
                tmp[64 * b : 64 * b + 60, 0:C] = rsq[k, 3 * a + b]
            w1[k, a] = tmp[:, 0:L].astype(F32).T.astype(BF16)
        for b in range(3):
            w2[k, b] = zero
            for a in range(3):
                w2[k, b, 64 * a : 64 * a + 60, 0:C] = rex[k, 3 * a + b]
        for dst, raw in ((gd, rgd), (gu, rgu)):
            dst[k] = jnp.zeros((8, L), F32)
            dst[k, 0:6, 0:C] = raw[k].astype(F32)

    def prepare_mlp(k):
        m1[k] = jnp.zeros((L, HL), BF16)
        m1[k, 0:C, 0:HID] = rm1[:, k, :]
        tmp[...] = jnp.zeros((L, HL), BF16)
        tmp[0:C, 0:HID] = rm2[:, k, :]
        m2[k] = tmp[...].astype(F32).T.astype(BF16)


    def copies_of(g, which):
        plan = [
            (row_s[g].at[0], row_r[g].at[0], (up, col)),
            (row_s[g].at[1], row_r[g].at[1], (down, col)),
            (col_s[g].at[0], col_r[g].at[0], (row, left)),
            (col_s[g].at[1], col_r[g].at[1], (row, right)),
            (cor_s[g].at[0], cor_r[g].at[0], (up, left)),
            (cor_s[g].at[1], cor_r[g].at[1], (up, right)),
            (cor_s[g].at[2], cor_r[g].at[2], (down, left)),
            (cor_s[g].at[3], cor_r[g].at[3], (down, right)),
        ]
        return [
            remote(s, d, hs.at[g, i], hr.at[g, i], p)
            for i in which
            for s, d, p in plan[i : i + 1]
        ]

    def send_rows(g):
        d0, n, _ = GROUPS[g]
        top = uf[d0 : d0 + n]
        low = uf[H - d0 - n : H - d0]
        pack(top, row_s[g].at[0])
        pack(low, row_s[g].at[1])
        pack(fold(top[:, 0:8]), cor_s[g].at[0])
        pack(fold(top[:, W - 8 : W]), cor_s[g].at[1])
        pack(fold(low[:, 0:8]), cor_s[g].at[2])
        pack(fold(low[:, W - 8 : W]), cor_s[g].at[3])
        low_half, top_half = copies_of(g, (6, 7, 1)), copies_of(g, (4, 5, 0))
        if g == 2:
            start(low_half)
        else:
            start(low_half[:2] + top_half[:2] + low_half[2:] + top_half[2:])
        return low_half, top_half

    def send_sides(g):
        pack(fold(uf[:, 0:8]), col_s[g].at[0])
        pack(fold(uf[:, W - 8 : W]), col_s[g].at[1])
        sides = copies_of(g, (2, 3))
        start(sides)
        return sides

    yes_up = jnp.where(row > 0, 1.0, 0.0)
    yes_down = jnp.where(row < ROWS - 1, 1.0, 0.0)
    yes_left = jnp.where(col > 0, 1.0, 0.0)
    yes_right = jnp.where(col < COLS - 1, 1.0, 0.0)

    def receive_rows(g, masked, whole, sides=(1, 0)):
        d0, n, _ = GROUPS[g]
        m = n // 2
        for which, lc, rc, at, keep in ((1, 3, 2, 8 - d0 - n, yes_up), (0, 1, 0, 24 + d0, yes_down)):
            if which not in sides:
                continue
            mid = unpack(row_r[g].at[which], n)
            lcorner = unfold(unpack(cor_r[g].at[lc], m))
            rcorner = unfold(unpack(cor_r[g].at[rc], m))
            if whole is not None:
                whole[at : at + n] = jnp.concatenate([lcorner, mid, rcorner], axis=1).astype(BF16)
            if masked is not None:
                masked[at : at + n] = jnp.concatenate(
                    [lcorner * (keep * yes_left), mid * keep, rcorner * (keep * yes_right)], axis=1
                ).astype(BF16)

    def receive_sides(g, masked, whole):
        lside = unfold(unpack(col_r[g].at[1], 8))
        rside = unfold(unpack(col_r[g].at[0], 8))
        first = un[:, 0:16].astype(F32)[:, 0:8]
        last = un[:, W - 16 : W].astype(F32)[:, 8:16]
        if whole is not None:
            whole[8:24, 0:16] = jnp.concatenate([lside, first], axis=1).astype(BF16)
            whole[8:24, 64:80] = jnp.concatenate([last, rside], axis=1).astype(BF16)
        if masked is not None:
            masked[8:24, 0:16] = jnp.concatenate([lside * yes_left, first], axis=1).astype(BF16)
            masked[8:24, 64:80] = jnp.concatenate([last, rside * yes_right], axis=1).astype(BF16)

    def settle(k):
        un[...] = uf[...].astype(BF16)
        inner = uf[:, 8:56].astype(BF16)
        ue[8:24, 16:64] = inner
        if k == 1:
            ua[8:24, 16:64] = inner

    def project(k, which, x):
        r, c, _ = x.shape
        y = dot(x.reshape(r * c, L), wqkv[k, which])
        if which == 0:
            y = y * QSCALE
        return y.astype(BF16).reshape(r, c, L)

    def project_plain(k, dsts):
        def step(i, carry):
            rows = pl.ds(i * 8, 8)
            x = un[rows]
            for which, dst in enumerate(dsts):
                dst[rows] = project(k, which, x)
            return carry

        lax.fori_loop(0, 2, step, 0)

    def project_inner(k, src, dsts):
        def step(i, carry):
            x = src[pl.ds(8 + 8 * i, 8), 16:64]
            for which, dst, base in dsts:
                dst[pl.ds(8 - base + 8 * i, 8), 16:64] = project(k, which, x)
            return carry

        lax.fori_loop(0, 2, step, 0)

    def project_sides(k, src, dsts):
        x = jnp.concatenate([src[8:24, 0:16], src[8:24, 64:80]], axis=1)
        for which, dst, base in dsts:
            y = project(k, which, x)
            dst[8 - base : 24 - base, 0:16] = y[:, 0:16]
            dst[8 - base : 24 - base, 64:80] = y[:, 16:32]

    def project_rows(k, src, n, sides=(1, 0)):
        for at in [(24, 8 - n)[side] for side in sides]:
            x = src[at : at + n]
            for which, dst in ((1, ke), (2, ve)):
                dst[at : at + n] = project(k, which, x)


    def plain_window(k):
        def step(w, carry):
            cols = pl.ds(pl.multiple_of(w * WIN, WIN), WIN)
            q = qs[:, cols].reshape(WIN * WIN, L)
            kk = ks[:, cols].reshape(WIN * WIN, L)
            vv = vs[:, cols].reshape(WIN * WIN, L)
            o = attend(q, kk, vv, HEADS)
            att[:, cols] = dot(o, wp[k]).reshape(WIN, WIN, L)
            return carry

        return step

    def shifted_windows(k, ry):
        lane = iota((1, 1, L), 2)
        qcol = iota((8, WIN, 1), 1) >= 8
        qpat = jnp.where(lane == C, 1.0, 0.0) + jnp.where(
            ((lane == C + 1) & ~qcol) | ((lane == C + 2) & qcol), 1.0, 0.0
        )
        krow = iota((WIN, WIN, 1), 0) >= 8
        kcol = iota((WIN, WIN, 1), 1) >= 8
        differs = krow if ry == 1 else ~krow
        brow = jnp.where(row == (ROWS - 1 if ry == 1 else 0), BIG, 0.0)
        rbias = jnp.where((lane == C) & differs, brow, 0.0)
        for w in range(5):
            cols = slice(w * WIN, (w + 1) * WIN)
            bias = rbias
            if w in (0, 4):
                bcol = jnp.where(col == (COLS - 1 if w == 4 else 0), BIG, 0.0)
                bias = bias + jnp.where(((lane == C + 1) & kcol) | ((lane == C + 2) & ~kcol), bcol, 0.0)
            q = (qe[8 * ry : 8 * ry + 8, cols].astype(F32) + qpat).astype(BF16)
            kk = (ke[WIN * ry : WIN * ry + WIN, cols].astype(F32) + bias).astype(BF16)
            vv = ve[WIN * ry : WIN * ry + WIN, cols]
            o = attend(q.reshape(8 * WIN, L), kk.reshape(WIN * WIN, L), vv.reshape(WIN * WIN, L), HEADS)
            oe[8 * ry : 8 * ry + 8, cols] = o.reshape(8, WIN, L)
        o = oe[8 * ry : 8 * ry + 8].reshape(8 * E, L)
        att[8 * ry : 8 * ry + 8] = dot(o, wp[k]).reshape(8, E, L)

    def cross_part(w, rows):
        lane = iota((1, 1, L), 2)
        qpat = jnp.where(lane == C, 1.0, 0.0)
        kcol = iota((1, 32, 1), 1)
        bias = jnp.where((lane == C) & ((kcol < 4) | (kcol >= 28)), BIG, 0.0)
        cols = slice(w * WIN, (w + 1) * WIN)
        wide = slice(w * WIN, w * WIN + 32)
        q = (qs[:, cols].astype(F32) + qpat).astype(BF16).reshape(WIN * WIN, L)
        kk = jnp.concatenate([ke[r, wide] for r in rows], axis=0)
        vv = jnp.concatenate([ve[r, wide] for r in rows], axis=0)
        n = kk.shape[0] * 32
        kk = (kk.astype(F32) + bias).astype(BF16).reshape(n, L)
        return attend_part(q, kk, vv.reshape(n, L), 2)

    def cross_near(windows):
        for w in windows:
            part = cross_part(w, (slice(8, 24),))
            for ref, value in zip((pn, pm, pd), part):
                ref[w] = value

    def cross_far(k):
        for w in range(4):
            far = cross_part(w, (slice(4, 8), slice(24, 28)))
            o = merge_parts(tuple(ref[w] for ref in (pn, pm, pd)), far)
            cols = slice(w * WIN, (w + 1) * WIN)
            x = st[:, cols].reshape(WIN * WIN, L) + dot(o, wp[k])
            u = layer_norm(x).astype(BF16)
            h = gelu(dot(u, m1[k])).astype(BF16)
            y = x + dot(h, m2[k])
            out[:, cols] = y.reshape(WIN, WIN, L)[:, :, :C].astype(out.dtype)


    def conv_in(k, spans):
        count = sum(n for _, n in spans)
        hcol = iota((count, E, 1), 1)
        lane = iota((1, 1, 128), 2)
        low = jnp.where(col == 0, 8, 0)
        high = jnp.where(col == COLS - 1, 72, E)
        at = iota((count, E, 1), 0) + spans[0][0]
        if len(spans) > 1:
            at = at + jnp.where(at >= spans[0][0] + spans[0][1], spans[1][0] - spans[0][1] - spans[0][0], 0)
        acc = None
        for a in range(3):
            x = jnp.concatenate([ue[6 + a + s : 6 + a + s + n] for s, n in spans], axis=0)
            y = dot(x.reshape(count * E, L), w1[k, a])
            acc = y if acc is None else acc + y
        r = acc.reshape(count, E, L)
        first, second = r[:, :, :128], r[:, :, 128:]
        s = pltpu.roll(first, 1, 1) + pltpu.roll(first, 64, 2) + pltpu.roll(second, E - 1, 1)
        ok = (hcol >= low) & (hcol < high) & (lane < 60)
        if len(spans) > 1:
            rlow = jnp.where(row == 0, 1, 0)
            rhigh = jnp.where(row == ROWS - 1, 17, 18)
            ok = ok & (at >= rlow) & (at < rhigh)
        g = jnp.where(ok, gelu(s), 0.0).astype(BF16).astype(F32)
        done = 0
        for s, n in spans:
            h32[s : s + n] = g[done : done + n]
            done += n

    def conv_first(k, g, sides, rows, also=None):
        whole = ua if k == 1 else None
        finish(sides)
        receive_sides(g, ue, whole)
        conv_in(k, ((2, 14),))
        if also is not None:
            also()
        finish(rows[0] + rows[1])
        receive_rows(g, ue, whole)
        conv_in(k, ((0, 2), (16, 2)))

    def conv_out(k):
        chunk = 8

        def step(i, carry):
            lead = h32[pl.ds(i * chunk, chunk)]
            mid = h32[pl.ds(i * chunk + 1, chunk)]
            tail = h32[pl.ds(i * chunk + 2, chunk)]
            x = jnp.concatenate([lead + pltpu.roll(mid, 64, 2), tail], axis=2)
            x = x.astype(BF16).reshape(chunk * E, L)
            r0 = dot(x, w2[k, 0]).reshape(chunk, E, L)
            r1 = dot(x, w2[k, 1]).reshape(chunk, E, L)
            r2 = dot(x, w2[k, 2]).reshape(chunk, E, L)
            y = (pltpu.roll(r0, 1, 1) + r1 + pltpu.roll(r2, E - 1, 1))[:, 8:72]
            ex[pl.ds(i * chunk, chunk)] = y
            return carry

        lax.fori_loop(0, H // chunk, step, 0)


    is_top, is_low = 1.0 - yes_up, 1.0 - yes_down
    is_left, is_right = 1.0 - yes_left, 1.0 - yes_right

    def expanded_sum(k):
        def over(x):
            return jnp.sum(jnp.sum(x, axis=0), axis=0, keepdims=True)

        every = over(h32[1:17, 8:72])
        top, low = over(h32[1:2, 8:72]) * is_top, over(h32[16:17, 8:72]) * is_low
        lead, tail = h32[1:17, 8:16][:, 0:1], h32[1:17, 64:72][:, 7:8]
        left_, right_ = over(lead) * is_left, over(tail) * is_right
        rows_out = (low, None, top)
        cols_out = (right_, None, left_)
        corner = {
            (0, 0): tail[15] * (is_low * is_right),
            (0, 2): lead[15] * (is_low * is_left),
            (2, 0): tail[0] * (is_top * is_right),
            (2, 2): lead[0] * (is_top * is_left),
        }
        total = None
        for b in range(3):
            s = []
            for a in range(3):
                v = every
                if rows_out[a] is not None:
                    v = v - rows_out[a]
                if cols_out[b] is not None:
                    v = v - cols_out[b]
                if (a, b) in corner:
                    v = v + corner[a, b]
                s.append(v)
            v = jnp.concatenate([s[0] + pltpu.roll(jnp.broadcast_to(s[1], (8, 128)), 64, 1)[0:1], s[2]], axis=1)
            first = v.astype(BF16).astype(F32)
            second = (v - first).astype(BF16).astype(F32)
            third = v - first - second
            x = jnp.concatenate([first, second, third, jnp.zeros((5, L), F32)], axis=0).astype(BF16)
            y = jnp.sum(dot(x, w2[k, b]), axis=0, keepdims=True)
            total = y if total is None else total + y
        return total

    def spread(k, part):
        arf[k, 0] = part

        def one(dr, dc):
            slot = dr * COLS + dc
            remote(arf.at[k, 0], arf.at[k, slot], asend.at[k], arecv.at[k], peer(dr, dc)).start()

        for_others(one)

    def gate(k):
        rest = arf.at[k, pl.ds(1, others)]
        remote(rest, rest, asend.at[k], arecv.at[k], (row, col)).wait()
        s = jnp.sum(arf[k], axis=0)
        pooled = s * (1.0 / (ROWS * COLS * H * W))
        squeezed = jnp.sum(gd[k] * pooled, axis=-1, keepdims=True)
        squeezed = jnp.maximum(squeezed, 0.0)
        z = jnp.sum(gu[k] * squeezed, axis=0, keepdims=True)
        return 1.0 / (1.0 + jnp.exp(-z))

    def feed_forward(k, scale, offset, pieces):
        parts = []
        for r, n, c, m in pieces:
            x = st[r : r + n, c : c + m] + att[r : r + n, offset + c : offset + c + m]
            if scale is not None:
                x = x + ex[r : r + n, c : c + m] * scale.reshape(1, 1, L)
            parts.append(x.reshape(n * m, L))
        x = jnp.concatenate(parts, axis=0)
        u = layer_norm(x).astype(BF16)
        h = gelu(dot(u, m1[k])).astype(BF16)
        y = x + dot(h, m2[k])
        v = layer_norm(y)
        done = 0
        for r, n, c, m in pieces:
            span = slice(done, done + n * m)
            done += n * m
            st[r : r + n, c : c + m] = y[span].reshape(n, m, L)
            uf[r : r + n, c : c + m] = v[span].reshape(n, m, L)

    def block_end(k, scale, offset, g):
        n = GROUPS[g][1]
        mid = H - 2 * n
        feed_forward(k, scale, offset, ((0, n, 0, W), (H - n, n, 0, W), (n, mid, 0, 8), (n, mid, W - 8, 8)))
        sides, rows = send_sides(g), send_rows(g)
        feed_forward(k, scale, offset, ((n, mid, 8, W - 16),))
        settle(k + 1)
        return rows, sides

    st[...] = jnp.zeros_like(st)
    st[:, :, :C] = tok[...].astype(F32)

    uf[...] = layer_norm(st[...])
    pl.semaphore_wait(barrier, len(peers))
    sides, rows = send_sides(0), send_rows(0)
    settle(0)
    for d in range(1, COLS):
        pl.semaphore_signal(ready, inc=1, device_id=peer(0, d), device_id_type=MESH)
    finish(loads)
    prepare_attention(0)
    prepare_conv(0)
    project_plain(0, (qs, ks, vs))
    prepare_mlp(0)
    prepare_attention(1)
    prepare_conv(1)
    prepare_mlp(1)
    conv_first(0, 0, sides, rows)
    part = expanded_sum(0)
    pl.semaphore_wait(ready, COLS - 1)
    spread(0, part)
    conv_out(0)
    lax.fori_loop(0, 4, plain_window(0), 0)
    prepare_attention(2)
    prepare_conv(2)
    rows, sides = block_end(0, gate(0), 0, 1)

    more = send_rows(2)
    project_inner(1, ua, ((0, qe, 8), (1, ke, 0), (2, ve, 0)))
    prepare_mlp(2)
    conv_first(1, 1, sides, rows, lambda: project_sides(1, ua, ((0, qe, 8), (1, ke, 0), (2, ve, 0))))
    spread(1, expanded_sum(1))
    start(more[1])
    conv_out(1)
    finish(more[0])
    receive_rows(2, None, ua, (1,))
    project_rows(1, ua, 8, (1,))
    shifted_windows(1, 0)
    finish(more[1])
    receive_rows(2, None, ua, (0,))
    project_rows(1, ua, 8, (0,))
    shifted_windows(1, 1)
    rows, sides = block_end(1, gate(1), 8, 3)

    project_plain(2, (qs, ks, vs))
    prepare_attention(3)
    prepare_mlp(3)
    conv_first(2, 3, sides, rows)
    spread(2, expanded_sum(2))
    conv_out(2)
    lax.fori_loop(0, 4, plain_window(2), 0)
    rows, sides = block_end(2, gate(2), 0, 4)

    project_plain(3, (qs,))
    project_inner(3, ue, ((1, ke, 0), (2, ve, 0)))
    cross_near((1, 2))
    finish(sides)
    receive_sides(4, ue, None)
    project_sides(3, ue, ((1, ke, 0), (2, ve, 0)))
    cross_near((0, 3))
    finish(rows[0] + rows[1])
    receive_rows(4, ue, None)
    project_rows(3, ue, 4)
    cross_far(3)


def local(tok, qkv, proj, squeeze, expand, down, up_, mlp_in, mlp_out, oqkv, oproj):
    args = (
        tok, qkv, proj, squeeze.transpose(0, 1, 3, 2), expand, down.transpose(0, 2, 1), up_,
        mlp_in.transpose(1, 0, 2), mlp_out.transpose(2, 0, 1), oqkv, oproj,
    )
    vmem = pl.BlockSpec(memory_space=pltpu.VMEM)
    hbm = pl.BlockSpec(memory_space=pltpu.HBM)
    scratch = [pltpu.VMEM(a.shape, a.dtype) for a in args[1:]]
    scratch += [
        pltpu.VMEM((4, 3, L, L), BF16),
        pltpu.VMEM((4, L, L), BF16),
        pltpu.VMEM((3, 3, L, L), BF16),
        pltpu.VMEM((3, 3, L, L), BF16),
        pltpu.VMEM((3, 8, L), F32),
        pltpu.VMEM((3, 8, L), F32),
        pltpu.VMEM((4, L, HL), BF16),
        pltpu.VMEM((4, HL, L), BF16),
        pltpu.VMEM((L, HL), BF16),
        pltpu.VMEM((4, WIN * WIN, L), F32),
        pltpu.VMEM((4, WIN * WIN, L), F32),
        pltpu.VMEM((4, WIN * WIN, L), F32),
        pltpu.VMEM((H, W, L), F32),
        pltpu.VMEM((H, W, L), F32),
        pltpu.VMEM((H, W, L), BF16),
        pltpu.VMEM((32, E, L), BF16),
        pltpu.VMEM((32, E, L), BF16),
        pltpu.VMEM((H, W, L), BF16),
        pltpu.VMEM((H, W, L), BF16),
        pltpu.VMEM((H, W, L), BF16),
        pltpu.VMEM((H, E, L), BF16),
        pltpu.VMEM((32, E, L), BF16),
        pltpu.VMEM((32, E, L), BF16),
        pltpu.VMEM((H, E, L), BF16),
        pltpu.VMEM((H, E, L), F32),
        pltpu.VMEM((H, W, L), F32),
        pltpu.VMEM((18, E, 128), F32),
        pltpu.VMEM((3, ROWS * COLS, 1, L), F32),
    ]
    for _, n, _ in GROUPS:
        for shape in ((2, packed(n), W, 128), (2, packed(8), 16, 128), (4, packed(n // 2), 16, 128)):
            scratch += [pltpu.VMEM(shape, BF16)] * 2
    dma = pltpu.SemaphoreType.DMA
    scratch += [dma((10,)), dma((len(GROUPS), 8)), dma((len(GROUPS), 8))]
    scratch += [dma((3,)), dma((3,)), pltpu.SemaphoreType.REGULAR]
    return pl.pallas_call(
        kernel,
        out_shape=jax.ShapeDtypeStruct((H, W, C), BF16),
        in_specs=[vmem] + [hbm] * 10,
        out_specs=vmem,
        scratch_shapes=scratch,
        compiler_params=pltpu.CompilerParams(
            collective_id=0, has_side_effects=True, vmem_limit_bytes=60 * 1024 * 1024
        ),
        name="blocks",
    )(*args)


def solution(mesh):
    placed = (P("row", "col", None),) + (P(),) * 10
    return jax.shard_map(
        local, mesh=mesh, in_specs=placed, out_specs=P("row", "col", None), check_vma=False
    )
```

```python
import jax
import jax.numpy as jnp
from jax import lax
from jax.experimental import pallas as pl
from jax.experimental.pallas import tpu as pltpu
from jax.sharding import PartitionSpec as P

C = 180
HEADS = 6
HD = C // HEADS
WIN = 16
L = 256
HID = 360
HL = 384
ROWS = 8
COLS = 16
H = 16
W = 64
E = 80
EPSILON = 1e-05
BIG = -1e30
QSCALE = HD ** (-0.5) * 1.4426950408889634
F32 = jnp.float32
BF16 = jnp.bfloat16
MESH = pl.DeviceIdType.MESH
GROUPS = ((0, 2, True), (0, 2, True), (2, 6, False), (0, 2, True), (0, 4, True))


def dot(a, b):
    return jnp.dot(a, b, preferred_element_type=F32)


def dot_t(a, b):
    return lax.dot_general(a, b, (((1,), (1,)), ((), ())), preferred_element_type=F32)


def gelu(v):
    return v * (1.0 + lax.erf(v * 0.7071067811865476)) * 0.5


def iota(shape, dim):
    return lax.broadcasted_iota(jnp.int32, shape, dim)


def layer_norm(x):
    nd = x.ndim
    inside = iota((1,) * (nd - 1) + (L,), nd - 1) < C
    mean = jnp.sum(x, axis=-1, keepdims=True) * (1.0 / C)
    centered = jnp.where(inside, x - mean, 0.0)
    spread = jnp.sum(centered * centered, axis=-1, keepdims=True) * (1.0 / C)
    return centered * lax.rsqrt(spread + EPSILON)


def attend_part(q, k, v, group):
    tq = q.shape[0]
    lane = iota((1, L), 1)
    num = top = den = None
    for first in range(0, HEADS, group):
        stacked = []
        for h in range(first, first + group):
            mask = ((lane >= h * HD) & (lane < h * HD + HD)) | (lane >= C)
            stacked.append(q * mask.astype(F32).astype(BF16))
        s = dot_t(jnp.concatenate(stacked, axis=0), k)
        m = jnp.max(s, axis=-1, keepdims=True)
        p = jnp.exp2(s - m)
        d = jnp.sum(p, axis=-1, keepdims=True)
        r = dot(p.astype(BF16), v)
        for i in range(group):
            span = slice(i * tq, (i + 1) * tq)
            here = lane >= (first + i) * HD
            wide = [r[span], jnp.broadcast_to(m[span], (tq, L)), jnp.broadcast_to(d[span], (tq, L))]
            if num is None:
                num, top, den = wide
            else:
                num, top, den = (jnp.where(here, x, y) for x, y in zip(wide, (num, top, den)))
    return num, top, den


def attend(q, k, v, group):
    num, _, den = attend_part(q, k, v, group)
    return (num / den).astype(BF16)


def merge_parts(a, b):
    (n0, m0, d0), (n1, m1, d1) = a, b
    m = jnp.maximum(m0, m1)
    c0, c1 = jnp.exp2(m0 - m), jnp.exp2(m1 - m)
    return ((n0 * c0 + n1 * c1) / (d0 * c0 + d1 * c1)).astype(BF16)


def packed(n):
    return n + (n + 1) // 2


def pack(x, ref):
    n = x.shape[0]
    half = (n + 1) // 2
    ref[0:n] = x[:, :, :128].astype(BF16)
    low = x[:half, :, 128:]
    if n > half:
        high = pltpu.roll(x[half:, :, 128:], 64, 2)
        if n < 2 * half:
            high = jnp.concatenate([high, jnp.zeros_like(low[:1])], axis=0)
        low = low + high
    ref[n : n + half] = low.astype(BF16)


def unpack(ref, n):
    half = (n + 1) // 2
    upper = iota((1, 1, 128), 2) < C - 128
    both = ref[n : n + half].astype(F32)
    b = jnp.where(upper, both, 0.0)
    if n > half:
        high = jnp.where(upper, pltpu.roll(both, 64, 2), 0.0)
        b = jnp.concatenate([b, high[: n - half]], axis=0)
    return jnp.concatenate([ref[0:n].astype(F32), b], axis=2)


def fold(x):
    m = x.shape[0] // 2
    return jnp.concatenate([x[:m], x[m:]], axis=1)


def unfold(x):
    return jnp.concatenate([x[:, :8], x[:, 8:]], axis=0)


def kernel(*refs):
    (
        tok, qkv_h, proj_h, sq_h, ex_h, gd_h, gu_h, m1_h, m2_h, oqkv_h, oproj_h, out,
        rqkv, rproj, rsq, rex, rgd, rgu, rm1, rm2, roqkv, roproj,
        wqkv, wp, w1, w2, gd, gu, m1, m2, tmp, pn, pm, pd,
        st, uf, un, ue, ua, qs, ks, vs, qe, ke, ve, oe, att, ex, h32, arf,
    ) = refs[:50]
    bufs = refs[50 : 50 + 6 * len(GROUPS)]
    wsem, hs, hr, asend, arecv, ready = refs[50 + 6 * len(GROUPS) :]
    row_s, row_r, col_s, col_r, cor_s, cor_r = (bufs[i :: 6] for i in range(6))
    row = lax.axis_index("row")
    col = lax.axis_index("col")
    up, down = lax.rem(row + ROWS - 1, ROWS), lax.rem(row + 1, ROWS)
    left, right = lax.rem(col + COLS - 1, COLS), lax.rem(col + 1, COLS)

    barrier = pltpu.get_barrier_semaphore()
    others = ROWS * COLS - 1

    def peer(dr, dc):
        return lax.rem(row + dr, ROWS), lax.rem(col + dc, COLS)

    def for_others(act):
        for dr in (4, 3, 5, 2, 6, 1, 7, 0):

            def step(i, carry, dr=dr):
                act(dr, lax.rem(i + COLS // 2, COLS))
                return carry

            if dr:
                lax.fori_loop(0, COLS, step, 0, unroll=4)
            else:
                lax.fori_loop(0, COLS // 2, step, 0)
                lax.fori_loop(COLS // 2 + 1, COLS, step, 0)

    peers = [peer(d, 0) for d in range(1, ROWS)] + [peer(0, d) for d in range(1, COLS)]
    peers += [(up, left), (up, right), (down, left), (down, right)]
    for p in peers:
        pl.semaphore_signal(barrier, inc=1, device_id=p, device_id_type=MESH)

    loads = [
        pltpu.make_async_copy(s, d, wsem.at[i])
        for i, (s, d) in enumerate(
            [
                (qkv_h, rqkv), (proj_h, rproj), (sq_h, rsq), (ex_h, rex), (gd_h, rgd),
                (gu_h, rgu), (m1_h, rm1), (m2_h, rm2), (oqkv_h, roqkv), (oproj_h, roproj),
            ]
        )
    ]
    for c in loads:
        c.start()

    def remote(src, dst, send, recv, peer):
        return pltpu.make_async_remote_copy(
            src_ref=src, dst_ref=dst, send_sem=send, recv_sem=recv, device_id=peer, device_id_type=MESH
        )

    def start(copies):
        for c in copies:
            c.start()

    def finish(copies):
        for c in copies:
            c.wait()


    def prepare_attention(k):
        w = rqkv.at[k] if k < 3 else roqkv
        zero = jnp.zeros((L, L), BF16)
        for i in range(3):
            wqkv[k, i] = zero
        whole = w[...]
        wqkv[k, 0, 0:C, 0:C] = w[:, 0:C]
        for i in range(1, 3):
            pick = (iota((3 * C, L), 0) == iota((3 * C, L), 1) + i * C) & (iota((3 * C, L), 1) < C)
            wqkv[k, i, 0:C] = dot(whole, jnp.where(pick, 1.0, 0.0).astype(BF16)).astype(BF16)
        wp[k] = zero
        wp[k, 0:C, 0:C] = rproj[k] if k < 3 else roproj[...]

    def prepare_conv(k):
        zero = jnp.zeros((L, L), BF16)
        for a in range(3):
            tmp[:, 0:L] = zero
            for b in range(3):
                tmp[64 * b : 64 * b + 60, 0:C] = rsq[k, 3 * a + b]
            w1[k, a] = tmp[:, 0:L].astype(F32).T.astype(BF16)
        for b in range(3):
            w2[k, b] = zero
            for a in range(3):
                w2[k, b, 64 * a : 64 * a + 60, 0:C] = rex[k, 3 * a + b]
        for dst, raw in ((gd, rgd), (gu, rgu)):
            dst[k] = jnp.zeros((8, L), F32)
            dst[k, 0:6, 0:C] = raw[k].astype(F32)

    def prepare_mlp(k):
        m1[k] = jnp.zeros((L, HL), BF16)
        m1[k, 0:C, 0:HID] = rm1[:, k, :]
        tmp[...] = jnp.zeros((L, HL), BF16)
        tmp[0:C, 0:HID] = rm2[:, k, :]
        m2[k] = tmp[...].astype(F32).T.astype(BF16)


    def copies_of(g, which):
        plan = [
            (row_s[g].at[0], row_r[g].at[0], (up, col)),
            (row_s[g].at[1], row_r[g].at[1], (down, col)),
            (col_s[g].at[0], col_r[g].at[0], (row, left)),
            (col_s[g].at[1], col_r[g].at[1], (row, right)),
            (cor_s[g].at[0], cor_r[g].at[0], (up, left)),
            (cor_s[g].at[1], cor_r[g].at[1], (up, right)),
            (cor_s[g].at[2], cor_r[g].at[2], (down, left)),
            (cor_s[g].at[3], cor_r[g].at[3], (down, right)),
        ]
        return [
            remote(s, d, hs.at[g, i], hr.at[g, i], p)
            for i in which
            for s, d, p in plan[i : i + 1]
        ]

    def send_rows(g):
        d0, n, _ = GROUPS[g]
        top = uf[d0 : d0 + n]
        low = uf[H - d0 - n : H - d0]
        pack(top, row_s[g].at[0])
        pack(low, row_s[g].at[1])
        pack(fold(top[:, 0:8]), cor_s[g].at[0])
        pack(fold(top[:, W - 8 : W]), cor_s[g].at[1])
        pack(fold(low[:, 0:8]), cor_s[g].at[2])
        pack(fold(low[:, W - 8 : W]), cor_s[g].at[3])
        low_half, top_half = copies_of(g, (6, 7, 1)), copies_of(g, (4, 5, 0))
        if g == 2:
            start(low_half)
        else:
            start(low_half[:2] + top_half[:2] + low_half[2:] + top_half[2:])
        return low_half, top_half

    def send_sides(g):
        pack(fold(uf[:, 0:8]), col_s[g].at[0])
        pack(fold(uf[:, W - 8 : W]), col_s[g].at[1])
        sides = copies_of(g, (2, 3))
        start(sides)
        return sides

    yes_up = jnp.where(row > 0, 1.0, 0.0)
    yes_down = jnp.where(row < ROWS - 1, 1.0, 0.0)
    yes_left = jnp.where(col > 0, 1.0, 0.0)
    yes_right = jnp.where(col < COLS - 1, 1.0, 0.0)

    def receive_rows(g, masked, whole, sides=(1, 0)):
        d0, n, _ = GROUPS[g]
        m = n // 2
        for which, lc, rc, at, keep in ((1, 3, 2, 8 - d0 - n, yes_up), (0, 1, 0, 24 + d0, yes_down)):
            if which not in sides:
                continue
            mid = unpack(row_r[g].at[which], n)
            lcorner = unfold(unpack(cor_r[g].at[lc], m))
            rcorner = unfold(unpack(cor_r[g].at[rc], m))
            if whole is not None:
                whole[at : at + n] = jnp.concatenate([lcorner, mid, rcorner], axis=1).astype(BF16)
            if masked is not None:
                masked[at : at + n] = jnp.concatenate(
                    [lcorner * (keep * yes_left), mid * keep, rcorner * (keep * yes_right)], axis=1
                ).astype(BF16)

    def receive_sides(g, masked, whole):
        lside = unfold(unpack(col_r[g].at[1], 8))
        rside = unfold(unpack(col_r[g].at[0], 8))
        first = un[:, 0:16].astype(F32)[:, 0:8]
        last = un[:, W - 16 : W].astype(F32)[:, 8:16]
        if whole is not None:
            whole[8:24, 0:16] = jnp.concatenate([lside, first], axis=1).astype(BF16)
            whole[8:24, 64:80] = jnp.concatenate([last, rside], axis=1).astype(BF16)
        if masked is not None:
            masked[8:24, 0:16] = jnp.concatenate([lside * yes_left, first], axis=1).astype(BF16)
            masked[8:24, 64:80] = jnp.concatenate([last, rside * yes_right], axis=1).astype(BF16)

    def settle(k):
        un[...] = uf[...].astype(BF16)
        inner = uf[:, 8:56].astype(BF16)
        ue[8:24, 16:64] = inner
        if k == 1:
            ua[8:24, 16:64] = inner

    def project(k, which, x):
        r, c, _ = x.shape
        y = dot(x.reshape(r * c, L), wqkv[k, which])
        if which == 0:
            y = y * QSCALE
        return y.astype(BF16).reshape(r, c, L)

    def project_plain(k, dsts):
        def step(i, carry):
            rows = pl.ds(i * 8, 8)
            x = un[rows]
            for which, dst in enumerate(dsts):
                dst[rows] = project(k, which, x)
            return carry

        lax.fori_loop(0, 2, step, 0)

    def project_inner(k, src, dsts):
        def step(i, carry):
            x = src[pl.ds(8 + 8 * i, 8), 16:64]
            for which, dst, base in dsts:
                dst[pl.ds(8 - base + 8 * i, 8), 16:64] = project(k, which, x)
            return carry

        lax.fori_loop(0, 2, step, 0)

    def project_sides(k, src, dsts):
        x = jnp.concatenate([src[8:24, 0:16], src[8:24, 64:80]], axis=1)
        for which, dst, base in dsts:
            y = project(k, which, x)
            dst[8 - base : 24 - base, 0:16] = y[:, 0:16]
            dst[8 - base : 24 - base, 64:80] = y[:, 16:32]

    def project_rows(k, src, n, sides=(1, 0)):
        for at in [(24, 8 - n)[side] for side in sides]:
            x = src[at : at + n]
            for which, dst in ((1, ke), (2, ve)):
                dst[at : at + n] = project(k, which, x)


    def plain_window(k):
        def step(w, carry):
            cols = pl.ds(pl.multiple_of(w * WIN, WIN), WIN)
            q = qs[:, cols].reshape(WIN * WIN, L)
            kk = ks[:, cols].reshape(WIN * WIN, L)
            vv = vs[:, cols].reshape(WIN * WIN, L)
            o = attend(q, kk, vv, HEADS)
            att[:, cols] = dot(o, wp[k]).reshape(WIN, WIN, L)
            return carry

        return step

    def shifted_windows(k, ry):
        lane = iota((1, 1, L), 2)
        qcol = iota((8, WIN, 1), 1) >= 8
        qpat = jnp.where(lane == C, 1.0, 0.0) + jnp.where(
            ((lane == C + 1) & ~qcol) | ((lane == C + 2) & qcol), 1.0, 0.0
        )
        krow = iota((WIN, WIN, 1), 0) >= 8
        kcol = iota((WIN, WIN, 1), 1) >= 8
        differs = krow if ry == 1 else ~krow
        brow = jnp.where(row == (ROWS - 1 if ry == 1 else 0), BIG, 0.0)
        rbias = jnp.where((lane == C) & differs, brow, 0.0)
        for w in range(5):
            cols = slice(w * WIN, (w + 1) * WIN)
            bias = rbias
            if w in (0, 4):
                bcol = jnp.where(col == (COLS - 1 if w == 4 else 0), BIG, 0.0)
                bias = bias + jnp.where(((lane == C + 1) & kcol) | ((lane == C + 2) & ~kcol), bcol, 0.0)
            q = (qe[8 * ry : 8 * ry + 8, cols].astype(F32) + qpat).astype(BF16)
            kk = (ke[WIN * ry : WIN * ry + WIN, cols].astype(F32) + bias).astype(BF16)
            vv = ve[WIN * ry : WIN * ry + WIN, cols]
            o = attend(q.reshape(8 * WIN, L), kk.reshape(WIN * WIN, L), vv.reshape(WIN * WIN, L), HEADS)
            oe[8 * ry : 8 * ry + 8, cols] = o.reshape(8, WIN, L)
        o = oe[8 * ry : 8 * ry + 8].reshape(8 * E, L)
        att[8 * ry : 8 * ry + 8] = dot(o, wp[k]).reshape(8, E, L)

    def cross_part(w, rows):
        lane = iota((1, 1, L), 2)
        qpat = jnp.where(lane == C, 1.0, 0.0)
        kcol = iota((1, 32, 1), 1)
        bias = jnp.where((lane == C) & ((kcol < 4) | (kcol >= 28)), BIG, 0.0)
        cols = slice(w * WIN, (w + 1) * WIN)
        wide = slice(w * WIN, w * WIN + 32)
        q = (qs[:, cols].astype(F32) + qpat).astype(BF16).reshape(WIN * WIN, L)
        kk = jnp.concatenate([ke[r, wide] for r in rows], axis=0)
        vv = jnp.concatenate([ve[r, wide] for r in rows], axis=0)
        n = kk.shape[0] * 32
        kk = (kk.astype(F32) + bias).astype(BF16).reshape(n, L)
        return attend_part(q, kk, vv.reshape(n, L), 2)

    def cross_near(windows):
        for w in windows:
            part = cross_part(w, (slice(8, 24),))
            for ref, value in zip((pn, pm, pd), part):
                ref[w] = value

    def cross_far(k):
        for w in range(4):
            far = cross_part(w, (slice(4, 8), slice(24, 28)))
            o = merge_parts(tuple(ref[w] for ref in (pn, pm, pd)), far)
            cols = slice(w * WIN, (w + 1) * WIN)
            x = st[:, cols].reshape(WIN * WIN, L) + dot(o, wp[k])
            u = layer_norm(x).astype(BF16)
            h = gelu(dot(u, m1[k])).astype(BF16)
            y = x + dot(h, m2[k])
            out[:, cols] = y.reshape(WIN, WIN, L)[:, :, :C].astype(out.dtype)


    def conv_in(k, spans):
        count = sum(n for _, n in spans)
        hcol = iota((count, E, 1), 1)
        lane = iota((1, 1, 128), 2)
        low = jnp.where(col == 0, 8, 0)
        high = jnp.where(col == COLS - 1, 72, E)
        at = iota((count, E, 1), 0) + spans[0][0]
        if len(spans) > 1:
            at = at + jnp.where(at >= spans[0][0] + spans[0][1], spans[1][0] - spans[0][1] - spans[0][0], 0)
        acc = None
        for a in range(3):
            x = jnp.concatenate([ue[6 + a + s : 6 + a + s + n] for s, n in spans], axis=0)
            y = dot(x.reshape(count * E, L), w1[k, a])
            acc = y if acc is None else acc + y
        r = acc.reshape(count, E, L)
        first, second = r[:, :, :128], r[:, :, 128:]
        s = pltpu.roll(first, 1, 1) + pltpu.roll(first, 64, 2) + pltpu.roll(second, E - 1, 1)
        ok = (hcol >= low) & (hcol < high) & (lane < 60)
        if len(spans) > 1:
            rlow = jnp.where(row == 0, 1, 0)
            rhigh = jnp.where(row == ROWS - 1, 17, 18)
            ok = ok & (at >= rlow) & (at < rhigh)
        g = jnp.where(ok, gelu(s), 0.0).astype(BF16).astype(F32)
        done = 0
        for s, n in spans:
            h32[s : s + n] = g[done : done + n]
            done += n

    def conv_first(k, g, sides, rows, also=None):
        whole = ua if k == 1 else None
        finish(sides)
        receive_sides(g, ue, whole)
        conv_in(k, ((2, 14),))
        if also is not None:
            also()
        finish(rows[0] + rows[1])
        receive_rows(g, ue, whole)
        conv_in(k, ((0, 2), (16, 2)))

    def conv_out(k):
        chunk = 8

        def step(i, carry):
            lead = h32[pl.ds(i * chunk, chunk)]
            mid = h32[pl.ds(i * chunk + 1, chunk)]
            tail = h32[pl.ds(i * chunk + 2, chunk)]
            x = jnp.concatenate([lead + pltpu.roll(mid, 64, 2), tail], axis=2)
            x = x.astype(BF16).reshape(chunk * E, L)
            r0 = dot(x, w2[k, 0]).reshape(chunk, E, L)
            r1 = dot(x, w2[k, 1]).reshape(chunk, E, L)
            r2 = dot(x, w2[k, 2]).reshape(chunk, E, L)
            y = (pltpu.roll(r0, 1, 1) + r1 + pltpu.roll(r2, E - 1, 1))[:, 8:72]
            ex[pl.ds(i * chunk, chunk)] = y
            return carry

        lax.fori_loop(0, H // chunk, step, 0)


    is_top, is_low = 1.0 - yes_up, 1.0 - yes_down
    is_left, is_right = 1.0 - yes_left, 1.0 - yes_right

    def expanded_sum(k):
        def over(x):
            return jnp.sum(jnp.sum(x, axis=0), axis=0, keepdims=True)

        every = over(h32[1:17, 8:72])
        top, low = over(h32[1:2, 8:72]) * is_top, over(h32[16:17, 8:72]) * is_low
        lead, tail = h32[1:17, 8:16][:, 0:1], h32[1:17, 64:72][:, 7:8]
        left_, right_ = over(lead) * is_left, over(tail) * is_right
        rows_out = (low, None, top)
        cols_out = (right_, None, left_)
        corner = {
            (0, 0): tail[15] * (is_low * is_right),
            (0, 2): lead[15] * (is_low * is_left),
            (2, 0): tail[0] * (is_top * is_right),
            (2, 2): lead[0] * (is_top * is_left),
        }
        total = None
        for b in range(3):
            s = []
            for a in range(3):
                v = every
                if rows_out[a] is not None:
                    v = v - rows_out[a]
                if cols_out[b] is not None:
                    v = v - cols_out[b]
                if (a, b) in corner:
                    v = v + corner[a, b]
                s.append(v)
            v = jnp.concatenate([s[0] + pltpu.roll(jnp.broadcast_to(s[1], (8, 128)), 64, 1)[0:1], s[2]], axis=1)
            first = v.astype(BF16).astype(F32)
            second = (v - first).astype(BF16).astype(F32)
            third = v - first - second
            x = jnp.concatenate([first, second, third, jnp.zeros((5, L), F32)], axis=0).astype(BF16)
            y = jnp.sum(dot(x, w2[k, b]), axis=0, keepdims=True)
            total = y if total is None else total + y
        return total

    def spread(k, part):
        arf[k, 0] = part

        def one(dr, dc):
            slot = dr * COLS + dc
            remote(arf.at[k, 0], arf.at[k, slot], asend.at[k], arecv.at[k], peer(dr, dc)).start()

        for_others(one)

    def gate(k):
        rest = arf.at[k, pl.ds(1, others)]
        remote(rest, rest, asend.at[k], arecv.at[k], (row, col)).wait()
        s = jnp.sum(arf[k], axis=0)
        pooled = s * (1.0 / (ROWS * COLS * H * W))
        squeezed = jnp.sum(gd[k] * pooled, axis=-1, keepdims=True)
        squeezed = jnp.maximum(squeezed, 0.0)
        z = jnp.sum(gu[k] * squeezed, axis=0, keepdims=True)
        return 1.0 / (1.0 + jnp.exp(-z))

    def feed_forward(k, scale, offset, pieces):
        parts = []
        for r, n, c, m in pieces:
            x = st[r : r + n, c : c + m] + att[r : r + n, offset + c : offset + c + m]
            if scale is not None:
                x = x + ex[r : r + n, c : c + m] * scale.reshape(1, 1, L)
            parts.append(x.reshape(n * m, L))
        x = jnp.concatenate(parts, axis=0)
        u = layer_norm(x).astype(BF16)
        h = gelu(dot(u, m1[k])).astype(BF16)
        y = x + dot(h, m2[k])
        v = layer_norm(y)
        done = 0
        for r, n, c, m in pieces:
            span = slice(done, done + n * m)
            done += n * m
            st[r : r + n, c : c + m] = y[span].reshape(n, m, L)
            uf[r : r + n, c : c + m] = v[span].reshape(n, m, L)

    def block_end(k, scale, offset, g):
        n = GROUPS[g][1]
        mid = H - 2 * n
        feed_forward(k, scale, offset, ((0, n, 0, W), (H - n, n, 0, W), (n, mid, 0, 8), (n, mid, W - 8, 8)))
        sides, rows = send_sides(g), send_rows(g)
        feed_forward(k, scale, offset, ((n, mid, 8, W - 16),))
        settle(k + 1)
        return rows, sides

    st[...] = jnp.zeros_like(st)
    st[:, :, :C] = tok[...].astype(F32)

    uf[...] = layer_norm(st[...])
    pl.semaphore_wait(barrier, len(peers))
    sides, rows = send_sides(0), send_rows(0)
    settle(0)
    for d in range(1, COLS):
        pl.semaphore_signal(ready, inc=1, device_id=peer(0, d), device_id_type=MESH)
    finish(loads)
    prepare_attention(0)
    prepare_conv(0)
    project_plain(0, (qs, ks, vs))
    prepare_mlp(0)
    prepare_attention(1)
    prepare_conv(1)
    prepare_mlp(1)
    conv_first(0, 0, sides, rows)
    part = expanded_sum(0)
    pl.semaphore_wait(ready, COLS - 1)
    spread(0, part)
    conv_out(0)
    lax.fori_loop(0, 4, plain_window(0), 0)
    rows, sides = block_end(0, gate(0), 0, 1)

    more = send_rows(2)
    project_inner(1, ua, ((0, qe, 8), (1, ke, 0), (2, ve, 0)))
    prepare_mlp(2)
    conv_first(1, 1, sides, rows, lambda: project_sides(1, ua, ((0, qe, 8), (1, ke, 0), (2, ve, 0))))
    spread(1, expanded_sum(1))
    start(more[1])
    conv_out(1)
    finish(more[0])
    receive_rows(2, None, ua, (1,))
    project_rows(1, ua, 8, (1,))
    shifted_windows(1, 0)
    prepare_attention(2)
    prepare_conv(2)
    finish(more[1])
    receive_rows(2, None, ua, (0,))
    project_rows(1, ua, 8, (0,))
    shifted_windows(1, 1)
    rows, sides = block_end(1, gate(1), 8, 3)

    project_plain(2, (qs, ks, vs))
    prepare_attention(3)
    prepare_mlp(3)
    conv_first(2, 3, sides, rows)
    spread(2, expanded_sum(2))
    conv_out(2)
    lax.fori_loop(0, 4, plain_window(2), 0)
    rows, sides = block_end(2, gate(2), 0, 4)

    project_plain(3, (qs,))
    project_inner(3, ue, ((1, ke, 0), (2, ve, 0)))
    cross_near((1, 2))
    finish(sides)
    receive_sides(4, ue, None)
    project_sides(3, ue, ((1, ke, 0), (2, ve, 0)))
    cross_near((0, 3))
    finish(rows[0] + rows[1])
    receive_rows(4, ue, None)
    project_rows(3, ue, 4)
    cross_far(3)


def local(tok, qkv, proj, squeeze, expand, down, up_, mlp_in, mlp_out, oqkv, oproj):
    args = (
        tok, qkv, proj, squeeze.transpose(0, 1, 3, 2), expand, down.transpose(0, 2, 1), up_,
        mlp_in.transpose(1, 0, 2), mlp_out.transpose(2, 0, 1), oqkv, oproj,
    )
    vmem = pl.BlockSpec(memory_space=pltpu.VMEM)
    hbm = pl.BlockSpec(memory_space=pltpu.HBM)
    scratch = [pltpu.VMEM(a.shape, a.dtype) for a in args[1:]]
    scratch += [
        pltpu.VMEM((4, 3, L, L), BF16),
        pltpu.VMEM((4, L, L), BF16),
        pltpu.VMEM((3, 3, L, L), BF16),
        pltpu.VMEM((3, 3, L, L), BF16),
        pltpu.VMEM((3, 8, L), F32),
        pltpu.VMEM((3, 8, L), F32),
        pltpu.VMEM((4, L, HL), BF16),
        pltpu.VMEM((4, HL, L), BF16),
        pltpu.VMEM((L, HL), BF16),
        pltpu.VMEM((4, WIN * WIN, L), F32),
        pltpu.VMEM((4, WIN * WIN, L), F32),
        pltpu.VMEM((4, WIN * WIN, L), F32),
        pltpu.VMEM((H, W, L), F32),
        pltpu.VMEM((H, W, L), F32),
        pltpu.VMEM((H, W, L), BF16),
        pltpu.VMEM((32, E, L), BF16),
        pltpu.VMEM((32, E, L), BF16),
        pltpu.VMEM((H, W, L), BF16),
        pltpu.VMEM((H, W, L), BF16),
        pltpu.VMEM((H, W, L), BF16),
        pltpu.VMEM((H, E, L), BF16),
        pltpu.VMEM((32, E, L), BF16),
        pltpu.VMEM((32, E, L), BF16),
        pltpu.VMEM((H, E, L), BF16),
        pltpu.VMEM((H, E, L), F32),
        pltpu.VMEM((H, W, L), F32),
        pltpu.VMEM((18, E, 128), F32),
        pltpu.VMEM((3, ROWS * COLS, 1, L), F32),
    ]
    for _, n, _ in GROUPS:
        for shape in ((2, packed(n), W, 128), (2, packed(8), 16, 128), (4, packed(n // 2), 16, 128)):
            scratch += [pltpu.VMEM(shape, BF16)] * 2
    dma = pltpu.SemaphoreType.DMA
    scratch += [dma((10,)), dma((len(GROUPS), 8)), dma((len(GROUPS), 8))]
    scratch += [dma((3,)), dma((3,)), pltpu.SemaphoreType.REGULAR]
    return pl.pallas_call(
        kernel,
        out_shape=jax.ShapeDtypeStruct((H, W, C), BF16),
        in_specs=[vmem] + [hbm] * 10,
        out_specs=vmem,
        scratch_shapes=scratch,
        compiler_params=pltpu.CompilerParams(
            collective_id=0, has_side_effects=True, vmem_limit_bytes=60 * 1024 * 1024
        ),
        name="blocks",
    )(*args)


def solution(mesh):
    placed = (P("row", "col", None),) + (P(),) * 10
    return jax.shard_map(
        local, mesh=mesh, in_specs=placed, out_specs=P("row", "col", None), check_vma=False
    )
```
